128 devices in a mesh: gx: 8 (over z_hi, x), gy: 4 (over z_lo, core), gz: 4 (over y).
Axes of the slice: x: 4, y: 4, z: 4 (z_hi: 2, z_lo: 2; z = z_hi * 2 + z_lo), core: 2. Of those that a mesh axis runs over, the one named last changes fastest.
Arguments:
- calcium: float32 [8, 256, 128, 512], P(None, 'gx', 'gz', 'gy'), may hold values from 0.1 to 3
- activation: float32 [8, 256, 128, 512], P(None, 'gx', 'gz', 'gy'), may hold values from 0 to 1
- element_first: int32 [256], replicated, may hold values from 0 to 63, as said below
- offset_first: float32 [256], replicated, may hold values from 0.1 to 0.9
- element_second: int32 [512], replicated, may hold values from 0 to 127, as said below
- offset_second: float32 [512], replicated, may hold values from 0.1 to 0.9
- element_third: int32 [128], replicated, may hold values from 0 to 31, as said below
- offset_third: float32 [128], replicated, may hold values from 0.1 to 0.9
- troponin: float32 [64, 32, 128], P('gx', ('gy', 'gz')), may hold values from 0 to 1
- tension: float32 [64, 32, 128], P('gx', ('gy', 'gz')), may hold values from 0 to 2
- unbind_rate: float32 [64, 32, 128], P('gx', ('gy', 'gz')), may hold values from 0.2 to 2
- relax_rate: float32 [64, 32, 128], P('gx', ('gy', 'gz')), may hold values from 0.5 to 4
Outputs:
- bound_fraction: float32 [64, 32, 128], P('gx', ('gy', 'gz'))
- active_tension: float32 [64, 32, 128], P('gx', ('gy', 'gz'))
The draws below stay inside these ranges and needn't reach their ends.
Inputs may be any that keep to these rules, and one draw needn't show every extreme that they name: `element_first`: never falling; the cells of each aligned block of 32 cells belong to that block's own 8 elements, each element holding at least one cell. `element_second`: never falling; the cells of each aligned block of 128 cells belong to that block's own 32 elements, each element holding at least one cell. `element_third`: never falling; the cells of each aligned block of 8 cells belong to that block's own 2 elements, each element holding at least one cell.
All inputs are finite; a program needn't handle non-finite values.
Results may differ from the reference program's by a relative error of at most 0.00005.
Values sent between devices are 32-bit elements.
No kernel may reach another device: no remote copies, remote signals or barrier semaphores. Data moves between devices by JAX's collectives and lax.ppermute only.
A program may use at most 64 MiB of HBM per device.

```python
import math
import jax
import jax.numpy as jnp
from jax import lax

EX_DEV = 8
EY_DEV = 32
EZ_BLK = 2
SUB = 8
FX_BLK = 32
FY_BLK = 128
FZ_BLK = 8
NXC = 64
NYC = 128
NZC = 32
NXF = 256
NYF = 512
NZF = 128


def block_elements(key, blocks, cells, elements):

    def single(block_key):
        scores = jax.random.permutation(block_key, cells - 1) + 1
        cut_points = jnp.sort(scores[:elements - 1])
        places = jnp.arange(cells)
        return jnp.sum((places[:, None] >= cut_points[None, :]).astype(jnp.int32), axis=1)
    block_keys = jax.random.split(key, blocks)
    within = jax.vmap(single)(block_keys)
    offsets = elements * jnp.arange(blocks)[:, None]
    return (within + offsets).reshape(-1).astype(jnp.int32)


def draw_element_first(key, part):
    return block_elements(jax.random.fold_in(key, 11), NXF // FX_BLK, FX_BLK, EX_DEV)


def draw_element_second(key, part):
    return block_elements(jax.random.fold_in(key, 23), NYF // FY_BLK, FY_BLK, EY_DEV)


def draw_element_third(key, part):
    return block_elements(jax.random.fold_in(key, 37), NZF // FZ_BLK, FZ_BLK, EZ_BLK)


def block_scale(rng, extent, cuts, least, largest):
    level, own = 1.0, jax.random.fold_in(rng, 6)
    for dim, shards_of in cuts:
        draws = jnp.exp(jax.random.uniform(jax.random.fold_in(own, dim), (shards_of,), jnp.float32, least / len(cuts), largest / len(cuts)))
        level = level * jnp.repeat(draws, extent[dim] // shards_of).reshape([-1 if axis == dim else 1 for axis in range(len(extent))])
    return level


def setup_inputs(seed: int = 0) -> dict:
    streams_of = jax.random.split(jax.random.key(seed), 13)
    return {
        "calcium": jnp.clip(jnp.exp(math.log(3.0) - 3.4011974 * jax.random.uniform(streams_of[0], (SUB, NXF, NZF, NYF), jnp.float32) ** block_scale(streams_of[0], (SUB, NXF, NZF, NYF), ((1, 8), (2, 4), (3, 4)), -0.2, 0.2)), 0.1, 3.0),
        "activation": jnp.clip(1.0 * jax.random.uniform(streams_of[1], (SUB, NXF, NZF, NYF), jnp.float32) ** block_scale(streams_of[1], (SUB, NXF, NZF, NYF), ((1, 8), (2, 4), (3, 4)), -0.2, 0.2), 0.0, 1.0),
        "element_first": draw_element_first(jax.random.fold_in(streams_of[12], 71), 0),
        "offset_first": jnp.clip(jax.random.uniform(streams_of[3], (NXF,), jnp.float32, 0.1, 0.9), 0.1, 0.9),
        "element_second": draw_element_second(jax.random.fold_in(streams_of[12], 71), 0),
        "offset_second": jnp.clip(jax.random.uniform(streams_of[5], (NYF,), jnp.float32, 0.1, 0.9), 0.1, 0.9),
        "element_third": draw_element_third(jax.random.fold_in(streams_of[12], 71), 0),
        "offset_third": jnp.clip(jax.random.uniform(streams_of[7], (NZF,), jnp.float32, 0.1, 0.9), 0.1, 0.9),
        "troponin": jnp.clip(1.0 * jax.random.uniform(streams_of[8], (NXC, NZC, NYC), jnp.float32) ** block_scale(streams_of[8], (NXC, NZC, NYC), ((0, 8), (1, 16)), -0.2, 0.2), 0.0, 1.0),
        "tension": jnp.clip(2.0 * jax.random.uniform(streams_of[9], (NXC, NZC, NYC), jnp.float32) ** block_scale(streams_of[9], (NXC, NZC, NYC), ((0, 8), (1, 16)), -0.2, 0.2), 0.0, 2.0),
        "unbind_rate": jnp.clip(jnp.exp(math.log(2.0) - 2.3025851 * jax.random.uniform(streams_of[10], (NXC, NZC, NYC), jnp.float32) ** block_scale(streams_of[10], (NXC, NZC, NYC), ((0, 8), (1, 16)), -0.2, 0.2)), 0.2, 2.0),
        "relax_rate": jnp.clip(jnp.exp(math.log(4.0) - 2.0794415 * jax.random.uniform(streams_of[11], (NXC, NZC, NYC), jnp.float32) ** block_scale(streams_of[11], (NXC, NZC, NYC), ((0, 8), (1, 16)), -0.2, 0.2)), 0.5, 4.0),
    }


highest = lax.Precision.HIGHEST
step_size = 0.2
bind_rate = 2.0
peak_tension = 2.0
half_square = 0.25


def weights(element, offset, count):
    node_ids = jnp.arange(count, dtype=jnp.int32)
    inside = element[None, :] == node_ids[:, None]
    following = element[None, :] + 1 == node_ids[:, None]
    raw_weights = jnp.where(inside, 1.0 - offset[None, :], 0.0) + jnp.where(following, offset[None, :], 0.0)
    return raw_weights / jnp.sum(raw_weights, axis=1, keepdims=True)


def restrict(field, weight_row, weight_depth, weight_col):
    section = jnp.einsum("ai,izy->azy", weight_row, field, precision=highest)
    section = jnp.einsum("bz,azy->aby", weight_depth, section, precision=highest)
    return jnp.einsum("cy,aby->abc", weight_col, section, precision=highest)


def reference(calcium, activation, element_first, offset_first, element_second, offset_second, element_third, offset_third, troponin, tension, unbind_rate, relax_rate):
    weight_row = weights(element_first, offset_first, NXC)
    weight_col = weights(element_second, offset_second, NYC)
    weight_depth = weights(element_third, offset_third, NZC)

    def single(index):
        return (restrict(calcium[index], weight_row, weight_depth, weight_col),
                restrict(activation[index], weight_row, weight_depth, weight_col))

    drive_calcium, drive_activation = lax.map(single, jnp.arange(SUB, dtype=jnp.int32))
    bound = troponin
    active = tension
    for substep in range(SUB):
        calcium_now = drive_calcium[substep]
        squared = calcium_now * calcium_now
        binding = squared / (squared + half_square)
        bound = bound + step_size * (bind_rate * binding * (1.0 - bound) - unbind_rate * bound)
        active = active + step_size * relax_rate * (peak_tension * drive_activation[substep] * bound - active)
    return bound, active
```

```python
import jax
import jax.numpy as jnp
from jax import lax
from jax.experimental import pallas as pl
from jax.experimental.pallas import tpu as pltpu
from jax.sharding import PartitionSpec as P

step_size = 0.2
bind_rate = 2.0
peak_tension = 2.0
half_square = 0.25

f32 = jnp.float32
bf16 = jnp.bfloat16
LANES = 128
SUBS = 8
NODES = 8
COLS = 32
ROWS = 88
BLOCK = 104
PIECE = 72


def hat(element, offset, first_node, rows):
    cells = element.shape[0]
    element = element.reshape(1, cells)
    offset = offset.reshape(1, cells)
    node = first_node + lax.broadcasted_iota(jnp.int32, (rows, cells), 0)
    raw = jnp.where(element == node, 1.0 - offset, 0.0) + jnp.where(
        element + 1 == node, offset, 0.0
    )
    return raw / jnp.sum(raw, axis=1, keepdims=True)


def halves(value):
    high = value.astype(bf16).astype(f32)
    return high, value - high


def lane_ids(rows):
    return lax.broadcasted_iota(jnp.int32, (rows, LANES), 1)


def pick_lanes(values, index):
    return jnp.take_along_axis(values, index, axis=1, mode="promise_in_bounds")


def restrict_kernel(
    calcium,
    activation,
    element_first,
    offset_first,
    element_second,
    offset_second,
    element_third,
    offset_third,
    blocks,
    edge,
    pair_weight,
    col_high,
    col_low,
    partials,
    packed,
):
    step = pl.program_id(0)
    gx, gy, gz = lax.axis_index("gx"), lax.axis_index("gy"), lax.axis_index("gz")

    @pl.when(step == 0)
    def _():
        first = hat(element_first[...], offset_first[...], gx * NODES, 16)
        own = jnp.where(gx >= 4, first[:, LANES:], first[:, :LANES])
        third = hat(element_third[...], offset_third[...], gz * NODES, 16)
        lane = lane_ids(16)
        depth = pick_lanes(third, gz * 32 + lane % 32)
        for tile in range(8):
            row = pick_lanes(own, lax.rem(gx, 4) * 32 + 4 * tile + lane // 32)
            parts = [depth[b : b + 1] * row[:NODES] for b in range(NODES + 1)]
            parts.append(row[NODES : NODES + 1] * depth[:NODES])
            corner = row[NODES : NODES + 1] * depth[NODES : NODES + 1]
            top = lax.broadcasted_iota(jnp.int32, (8, LANES), 0) == 0
            parts.append(jnp.where(top, corner, 0.0))
            both = jnp.concatenate(halves(jnp.concatenate(parts, 0)), 0)
            pair_weight[:, tile * LANES : (tile + 1) * LANES] = both.astype(bf16)

    @pl.when(step == 2)
    def _():
        second = hat(element_second[...], offset_second[...], gy * COLS, 40)
        own = second[:, :LANES]
        for chunk in range(1, 4):
            piece = second[:, chunk * LANES : (chunk + 1) * LANES]
            own = jnp.where(gy == chunk, piece, own)
        full = jnp.concatenate([own, jnp.zeros((LANES - 40, LANES), f32)], 0)
        turned = full.T
        lane = lane_ids(LANES)
        for group in range(4):
            start = group * COLS
            main = turned if start == 0 else pltpu.roll(turned, start, 1)
            main = jnp.where(lane // COLS == group, main, 0.0)
            shift = (start - COLS) % LANES
            extra = turned if shift == 0 else pltpu.roll(turned, shift, 1)
            extra = jnp.where(lane == start, extra, 0.0)
            high, low = halves(jnp.concatenate([main, extra], 1))
            rows = slice(group * LANES, (group + 1) * LANES)
            col_high[rows] = high.astype(bf16)
            col_low[rows] = low.astype(bf16)

    cells = 32 * 32
    field = jnp.concatenate(
        [calcium[0].reshape(cells, LANES), activation[0].reshape(cells, LANES)], 1
    )
    high, low = halves(field)
    upper = jnp.dot(pair_weight[...], high.astype(bf16), preferred_element_type=f32)
    lower = jnp.dot(pair_weight[:96], low.astype(bf16), preferred_element_type=f32)
    section = upper[:ROWS] + upper[ROWS:] + lower[:ROWS]
    group = lax.rem(step, 4)
    partials[group, :ROWS] = section[:, :LANES]
    partials[group, ROWS:] = section[:, LANES:]

    def columns():
        whole = jnp.concatenate([partials[g] for g in range(4)], 1)
        high, low = halves(whole)
        high, low = high.astype(bf16), low.astype(bf16)
        return (
            jnp.dot(high, col_high[...], preferred_element_type=f32)
            + jnp.dot(low, col_high[...], preferred_element_type=f32)
            + jnp.dot(high, col_low[...], preferred_element_type=f32)
        )

    @pl.when(step == 3)
    def _():
        packed[...] = columns()

    @pl.when(step == SUBS - 1)
    def _():
        first, last = packed[...], columns()
        quads = [first[:ROWS], last[:ROWS], first[ROWS:], last[ROWS:]]
        main = [q[:, :LANES] for q in quads]
        extra = quads[0][:, LANES:]
        for j in range(1, 4):
            extra = extra + pltpu.roll(quads[j][:, LANES:], j, 1)
        for k in range(4):
            tail = None
            for p, plane in enumerate((2 * k, 2 * k + 1, NODES)):
                rows = slice(plane * 8, plane * 8 + 8)
                for j in range(4):
                    start = j * 24 + p * 8
                    blocks[k, start : start + 8] = main[j][rows]
                piece = extra[rows]
                piece = piece if p == 0 else pltpu.roll(piece, 4 * p, 1)
                tail = piece if tail is None else tail + piece
            blocks[k, 96:104] = tail
        for j in range(4):
            edge[j * 8 : j * 8 + 8] = main[j][72:80]
        corners = [m[80:81] for m in main] + [extra[80:81]]
        edge[32:40] = jnp.concatenate(corners + [jnp.zeros((3, LANES), f32)], 0)
        edge[40:48] = extra[72:80]


def route_kernel(blocks, incoming, *outs):
    gz = lax.axis_index("gz")
    top = lax.broadcasted_iota(jnp.int32, (8, LANES), 0) == 0
    for k in range(4):
        which = lax.rem(gz + k, 4)
        out = outs[k]
        tail = None
        for p in range(3):
            for j in range(4):
                start = j * 24 + p * 8
                if p < 2:
                    row = incoming[pl.ds(j * 8 + 2 * which + p, 1), :]
                else:
                    row = incoming[32 + j : 33 + j, :]
                out[start : start + 8] = blocks[which, start : start + 8] + jnp.where(
                    top, row, 0.0
                )
            if p < 2:
                row = incoming[pl.ds(40 + 2 * which + p, 1), :]
            else:
                row = incoming[36:37, :]
            row = jnp.where(top, row, 0.0)
            row = row if p == 0 else pltpu.roll(row, 4 * p, 1)
            tail = row if tail is None else tail + row
        out[96:104] = blocks[which, 96:104] + tail


def combine_kernel(own, one, two, three, *rest):
    outs, slabs = rest[:4], rest[4]
    gy, gz = lax.axis_index("gy"), lax.axis_index("gz")
    for k, message in enumerate((own, one, two, three)):
        slabs[lax.rem(gz + 4 - k, 4)] = message[...]
    lane = lane_ids(8)
    for k in range(4):
        slab = lax.rem(gy + k, 4)
        before = lax.rem(slab + 3, 4)
        joins = jnp.logical_and(gz == 0, slab > 0)
        out = outs[k]
        for j in range(4):
            start = j * 24
            plane = slabs[before, start + 16 : start + 24]
            out[j * 16 : j * 16 + 8] = slabs[slab, start : start + 8] + jnp.where(
                joins, plane, 0.0
            )
            out[j * 16 + 8 : j * 16 + 16] = slabs[slab, start + 8 : start + 16]
        tail = pltpu.roll(slabs[before, 96:104], LANES - 8, 1)
        tail = jnp.where(jnp.logical_and(joins, lane % COLS < 4), tail, 0.0)
        out[64:72] = slabs[slab, 96:104] + tail


def tension_kernel(
    own, one, two, three, troponin, tension, unbind, relax, bound_out, active_out, chunks
):
    gy = lax.axis_index("gy")
    for k, message in enumerate((own, one, two, three)):
        chunks[lax.rem(gy + 4 - k, 4)] = message[...]
    lane = lane_ids(8)
    pieces = [chunks[c] for c in range(4)]

    def turn(value, shift):
        shift = shift % LANES
        return value if shift == 0 else pltpu.roll(value, shift, 1)

    def drive(f, substep, plane):
        half, group = divmod(substep, 4)
        j = 2 * f + half
        start = j * 16 + plane * 8
        total = None
        for c in range(4):
            part = turn(pieces[c][start : start + 8], COLS * (c - group))
            total = part if total is None else jnp.where(lane // COLS == c, part, total)
        for c in range(3):
            shift = COLS * (c + 1) - (COLS * group + 4 * plane + j)
            part = turn(pieces[c][64:72], shift)
            total = total + jnp.where(lane == COLS * (c + 1), part, 0.0)
        return total

    for plane in range(2):
        bound = troponin[:, plane, :]
        active = tension[:, plane, :]
        unbinding = unbind[:, plane, :]
        relaxing = step_size * relax[:, plane, :]
        for substep in range(SUBS):
            calcium_now = drive(0, substep, plane)
            squared = calcium_now * calcium_now
            binding = squared / (squared + half_square)
            bound = bound + step_size * (
                bind_rate * binding * (1.0 - bound) - unbinding * bound
            )
            active = active + relaxing * (
                peak_tension * drive(1, substep, plane) * bound - active
            )
        bound_out[:, plane, :] = bound
        active_out[:, plane, :] = active


def exchange(messages, axis):
    received = [messages[0]]
    for k in range(1, 4):
        pairs = [(i, (i + k) % 4) for i in range(4)]
        received.append(lax.ppermute(messages[k], axis, pairs))
    return received


def per_device(
    calcium,
    activation,
    element_first,
    offset_first,
    element_second,
    offset_second,
    element_third,
    offset_third,
    troponin,
    tension,
    unbind_rate,
    relax_rate,
):
    field_spec = pl.BlockSpec((1, 32, 32, LANES), lambda s: (s, 0, 0, 0))
    line = lambda n: pl.BlockSpec((n,), lambda s: (0,))
    blocks, edge = pl.pallas_call(
        restrict_kernel,
        grid=(SUBS,),
        in_specs=[
            field_spec,
            field_spec,
            line(256),
            line(256),
            line(512),
            line(512),
            line(128),
            line(128),
        ],
        out_specs=[
            pl.BlockSpec((4, BLOCK, LANES), lambda s: (0, 0, 0)),
            pl.BlockSpec((48, LANES), lambda s: (0, 0)),
        ],
        out_shape=[
            jax.ShapeDtypeStruct((4, BLOCK, LANES), f32),
            jax.ShapeDtypeStruct((48, LANES), f32),
        ],
        scratch_shapes=[
            pltpu.VMEM((2 * ROWS, 1024), bf16),
            pltpu.VMEM((512, 256), bf16),
            pltpu.VMEM((512, 256), bf16),
            pltpu.VMEM((4, 2 * ROWS, LANES), f32),
            pltpu.VMEM((2 * ROWS, 256), f32),
        ],
        compiler_params=pltpu.CompilerParams(dimension_semantics=("arbitrary",)),
        name="restrict",
    )(
        calcium,
        activation,
        element_first,
        offset_first,
        element_second,
        offset_second,
        element_third,
        offset_third,
    )
    incoming = lax.ppermute(edge, "gx", [(i, i + 1) for i in range(7)])
    message = jax.ShapeDtypeStruct((BLOCK, LANES), f32)
    messages = pl.pallas_call(route_kernel, out_shape=[message] * 4, name="route")(
        blocks, incoming
    )
    messages = exchange(messages, "gz")
    piece = jax.ShapeDtypeStruct((PIECE, LANES), f32)
    pieces = pl.pallas_call(
        combine_kernel,
        out_shape=[piece] * 4,
        scratch_shapes=[pltpu.VMEM((4, BLOCK, LANES), f32)],
        name="combine",
    )(*messages)
    pieces = exchange(pieces, "gy")
    result = jax.ShapeDtypeStruct(troponin.shape, f32)
    return pl.pallas_call(
        tension_kernel,
        out_shape=[result, result],
        scratch_shapes=[pltpu.VMEM((4, PIECE, LANES), f32)],
        name="tension",
    )(*pieces, troponin, tension, unbind_rate, relax_rate)


def solution(mesh):
    node_spec = P("gx", ("gy", "gz"), None)
    return jax.shard_map(
        per_device,
        mesh=mesh,
        in_specs=(P(None, "gx", "gz", "gy"),) * 2 + (P(),) * 6 + (node_spec,) * 4,
        out_specs=(node_spec, node_spec),
        check_vma=False,
    )
```

```python
import jax
import jax.numpy as jnp
from jax import lax
from jax.experimental import pallas as pl
from jax.experimental.pallas import tpu as pltpu
from jax.sharding import PartitionSpec as P

step_size = 0.2
bind_rate = 2.0
peak_tension = 2.0
half_square = 0.25

f32 = jnp.float32
bf16 = jnp.bfloat16
LANES = 128
SUBS = 8
NODES = 8
COLS = 32
ROWS = 72
BLOCK = 104
PIECE = 72


def hat(element, offset, first_node, rows):
    cells = element.shape[0]
    element = element.reshape(1, cells)
    offset = offset.reshape(1, cells)
    node = first_node + lax.broadcasted_iota(jnp.int32, (rows, cells), 0)
    raw = jnp.where(element == node, 1.0 - offset, 0.0) + jnp.where(
        element + 1 == node, offset, 0.0
    )
    return raw / jnp.sum(raw, axis=1, keepdims=True)


def halves(value):
    high = value.astype(bf16).astype(f32)
    return high, value - high


def lane_ids(rows):
    return lax.broadcasted_iota(jnp.int32, (rows, LANES), 1)


def pick_lanes(values, index):
    return jnp.take_along_axis(values, index, axis=1, mode="promise_in_bounds")


def edge_kernel(
    calcium,
    activation,
    element_first,
    offset_first,
    element_second,
    offset_second,
    element_third,
    offset_third,
    edge,
    pair_weight,
    col_high,
    col_low,
    elements_1,
    offsets_1,
    elements_2,
    offsets_2,
    elements_3,
    offsets_3,
    cells,
    sums,
    small_sems,
    cell_sems,
):
    gx, gy, gz = lax.axis_index("gx"), lax.axis_index("gy"), lax.axis_index("gz")
    small = [
        (element_first, elements_1),
        (offset_first, offsets_1),
        (element_third, elements_3),
        (offset_third, offsets_3),
        (element_second, elements_2),
        (offset_second, offsets_2),
    ]
    loads = [
        pltpu.make_async_copy(source, target, small_sems.at[n])
        for n, (source, target) in enumerate(small)
    ]
    for load in loads:
        load.start()
    loads[0].wait()

    place = lax.broadcasted_iota(jnp.int32, (1, 256), 1)
    earlier = jnp.logical_and(
        place // 32 == gx, elements_1[...].reshape(1, 256) < gx * NODES + NODES - 1
    )
    begin = jnp.sum(jnp.where(earlier, 1.0, 0.0)).astype(jnp.int32)

    def cell_copies(x):
        return [
            pltpu.make_async_copy(field.at[:, x], cells.at[f, x], cell_sems.at[f, x])
            for f, field in enumerate((calcium, activation))
        ]

    def start(x, carry):
        for copy in cell_copies(x):
            copy.start()
        return carry

    lax.fori_loop(begin, 32, start, 0)
    loads[1].wait()
    loads[2].wait()
    loads[3].wait()

    first = hat(elements_1[...], offsets_1[...], gx * NODES, 16)
    own = jnp.where(gx >= 4, first[:, LANES:], first[:, :LANES])
    third = hat(elements_3[...], offsets_3[...], gz * NODES, 16)
    lane = lane_ids(16)
    depth = pick_lanes(third, gz * 32 + lane % 32)
    for tile in range(8):
        row = pick_lanes(own, lax.rem(gx, 4) * 32 + 4 * tile + lane // 32)
        parts = [depth[b : b + 1] * row[:NODES] for b in range(NODES + 1)]
        both = jnp.concatenate(halves(jnp.concatenate(parts, 0)), 0)
        pair_weight[:, tile * LANES : (tile + 1) * LANES] = both.astype(bf16)

    loads[4].wait()
    loads[5].wait()
    second = hat(elements_2[...], offsets_2[...], gy * COLS, 40)
    chunk = second[:, :LANES]
    for c in range(1, 4):
        chunk = jnp.where(gy == c, second[:, c * LANES : (c + 1) * LANES], chunk)
    full = jnp.concatenate([chunk, jnp.zeros((LANES - 40, LANES), f32)], 0)
    turned = full.T
    lane = lane_ids(LANES)
    for group in range(4):
        first_lane = group * COLS
        main = turned if group == 0 else pltpu.roll(turned, first_lane, 1)
        main = jnp.where(lane // COLS == group, main, 0.0)
        shift = (first_lane - COLS) % LANES
        extra = turned if shift == 0 else pltpu.roll(turned, shift, 1)
        extra = jnp.where(lane == first_lane, extra, 0.0)
        high, low = halves(jnp.concatenate([main, extra], 1))
        rows = slice(group * LANES, (group + 1) * LANES)
        col_high[rows] = high.astype(bf16)
        col_low[rows] = low.astype(bf16)

    def finish(x, carry):
        for copy in cell_copies(x):
            copy.wait()
        return carry

    lax.fori_loop(begin, 32, finish, 0)
    layer = jnp.broadcast_to(own[NODES : NODES + 1], (8, LANES))
    for f in range(2):
        for half in range(2):

            def add(x, total):
                index = jnp.full((8, LANES), lax.rem(gx, 4) * 32 + x, jnp.int32)
                weight = pick_lanes(layer, index)
                values = cells[f, x, 4 * half : 4 * half + 4].reshape(16, 8, LANES)
                return total + weight[None] * values

            total = lax.fori_loop(begin, 32, add, jnp.zeros((16, 8, LANES), f32))
            total = total.reshape(4, 32, LANES)
            for g in range(4):
                column = (f * 8 + half * 4 + g) * LANES
                sums[:, column : column + LANES] = total[g]

    depth_high, depth_low = halves(depth[:, :32])
    weights = jnp.concatenate([depth_high, depth_low], 0).astype(bf16)
    high, low = halves(sums[...])
    upper = jnp.dot(weights, high.astype(bf16), preferred_element_type=f32)
    lower = jnp.dot(weights[:16], low.astype(bf16), preferred_element_type=f32)
    planes = upper[:16] + upper[16:] + lower
    whole = jnp.concatenate([planes[:, j * 512 : (j + 1) * 512] for j in range(4)], 0)
    result = columns(whole, col_high, col_low)
    quads = [result[j * 16 : j * 16 + 16] for j in range(4)]
    extra = quads[0][:, LANES:]
    for j in range(1, 4):
        extra = extra + pltpu.roll(quads[j][:, LANES:], j, 1)
    for j in range(4):
        edge[j * 8 : j * 8 + 8] = quads[j][:8, :LANES]
    corners = [q[8:9, :LANES] for q in quads] + [extra[8:9]]
    edge[32:40] = jnp.concatenate(corners + [jnp.zeros((3, LANES), f32)], 0)
    edge[40:48] = extra[:8]


def columns(whole, col_high, col_low):
    high, low = halves(whole)
    high, low = high.astype(bf16), low.astype(bf16)
    return (
        jnp.dot(high, col_high[...], preferred_element_type=f32)
        + jnp.dot(low, col_high[...], preferred_element_type=f32)
        + jnp.dot(high, col_low[...], preferred_element_type=f32)
    )


def restrict_kernel(
    calcium, activation, pair_weight, col_high, col_low, blocks, partials, packed
):
    step = pl.program_id(0)
    cells = 32 * 32
    field = jnp.concatenate(
        [calcium[0].reshape(cells, LANES), activation[0].reshape(cells, LANES)], 1
    )
    high, low = halves(field)
    upper = jnp.dot(pair_weight[...], high.astype(bf16), preferred_element_type=f32)
    lower = jnp.dot(pair_weight[:80], low.astype(bf16), preferred_element_type=f32)
    section = upper[:ROWS] + upper[ROWS:] + lower[:ROWS]
    group = lax.rem(step, 4)
    partials[group, :ROWS] = section[:, :LANES]
    partials[group, ROWS:] = section[:, LANES:]

    def contract():
        whole = jnp.concatenate([partials[g] for g in range(4)], 1)
        return columns(whole, col_high, col_low)

    @pl.when(step == 3)
    def _():
        packed[...] = contract()

    @pl.when(step == SUBS - 1)
    def _():
        first, last = packed[...], contract()
        quads = [first[:ROWS], last[:ROWS], first[ROWS:], last[ROWS:]]
        main = [q[:, :LANES] for q in quads]
        extra = quads[0][:, LANES:]
        for j in range(1, 4):
            extra = extra + pltpu.roll(quads[j][:, LANES:], j, 1)
        for k in range(4):
            tail = None
            for p, plane in enumerate((2 * k, 2 * k + 1, NODES)):
                rows = slice(plane * 8, plane * 8 + 8)
                for j in range(4):
                    start = j * 24 + p * 8
                    blocks[k, start : start + 8] = main[j][rows]
                piece = extra[rows]
                piece = piece if p == 0 else pltpu.roll(piece, 4 * p, 1)
                tail = piece if tail is None else tail + piece
            blocks[k, 96:104] = tail


def route_kernel(blocks, incoming, *outs):
    gz = lax.axis_index("gz")
    top = lax.broadcasted_iota(jnp.int32, (8, LANES), 0) == 0
    for k in range(4):
        which = lax.rem(gz + k, 4)
        out = outs[k]
        tail = None
        for p in range(3):
            for j in range(4):
                start = j * 24 + p * 8
                if p < 2:
                    row = incoming[pl.ds(j * 8 + 2 * which + p, 1), :]
                else:
                    row = incoming[32 + j : 33 + j, :]
                out[start : start + 8] = blocks[which, start : start + 8] + jnp.where(
                    top, row, 0.0
                )
            if p < 2:
                row = incoming[pl.ds(40 + 2 * which + p, 1), :]
            else:
                row = incoming[36:37, :]
            row = jnp.where(top, row, 0.0)
            row = row if p == 0 else pltpu.roll(row, 4 * p, 1)
            tail = row if tail is None else tail + row
        out[96:104] = blocks[which, 96:104] + tail


def combine_kernel(own, one, two, three, *rest):
    outs, slabs = rest[:4], rest[4]
    gy, gz = lax.axis_index("gy"), lax.axis_index("gz")
    for k, message in enumerate((own, one, two, three)):
        slabs[lax.rem(gz + 4 - k, 4)] = message[...]
    lane = lane_ids(8)
    for k in range(4):
        slab = lax.rem(gy + k, 4)
        before = lax.rem(slab + 3, 4)
        joins = jnp.logical_and(gz == 0, slab > 0)
        out = outs[k]
        for j in range(4):
            start = j * 24
            plane = slabs[before, start + 16 : start + 24]
            out[j * 16 : j * 16 + 8] = slabs[slab, start : start + 8] + jnp.where(
                joins, plane, 0.0
            )
            out[j * 16 + 8 : j * 16 + 16] = slabs[slab, start + 8 : start + 16]
        tail = pltpu.roll(slabs[before, 96:104], LANES - 8, 1)
        tail = jnp.where(jnp.logical_and(joins, lane % COLS < 4), tail, 0.0)
        out[64:72] = slabs[slab, 96:104] + tail


def tension_kernel(
    own, one, two, three, troponin, tension, unbind, relax, bound_out, active_out, chunks
):
    gy = lax.axis_index("gy")
    for k, message in enumerate((own, one, two, three)):
        chunks[lax.rem(gy + 4 - k, 4)] = message[...]
    lane = lane_ids(8)
    pieces = [chunks[c] for c in range(4)]

    def turn(value, shift):
        shift = shift % LANES
        return value if shift == 0 else pltpu.roll(value, shift, 1)

    def drive(f, substep, plane):
        half, group = divmod(substep, 4)
        j = 2 * f + half
        start = j * 16 + plane * 8
        total = None
        for c in range(4):
            part = turn(pieces[c][start : start + 8], COLS * (c - group))
            total = part if total is None else jnp.where(lane // COLS == c, part, total)
        for c in range(3):
            shift = COLS * (c + 1) - (COLS * group + 4 * plane + j)
            part = turn(pieces[c][64:72], shift)
            total = total + jnp.where(lane == COLS * (c + 1), part, 0.0)
        return total

    for plane in range(2):
        bound = troponin[:, plane, :]
        active = tension[:, plane, :]
        unbinding = unbind[:, plane, :]
        relaxing = step_size * relax[:, plane, :]
        for substep in range(SUBS):
            calcium_now = drive(0, substep, plane)
            squared = calcium_now * calcium_now
            binding = squared / (squared + half_square)
            bound = bound + step_size * (
                bind_rate * binding * (1.0 - bound) - unbinding * bound
            )
            active = active + relaxing * (
                peak_tension * drive(1, substep, plane) * bound - active
            )
        bound_out[:, plane, :] = bound
        active_out[:, plane, :] = active


def exchange(messages, axis):
    received = [messages[0]]
    for k in range(1, 4):
        pairs = [(i, (i + k) % 4) for i in range(4)]
        received.append(lax.ppermute(messages[k], axis, pairs))
    return received


def per_device(
    calcium,
    activation,
    element_first,
    offset_first,
    element_second,
    offset_second,
    element_third,
    offset_third,
    troponin,
    tension,
    unbind_rate,
    relax_rate,
):
    line = lambda n, kind: pltpu.VMEM((n,), kind)
    vectors = (
        element_first,
        offset_first,
        element_second,
        offset_second,
        element_third,
        offset_third,
    )
    far = [
        pltpu.with_memory_space_constraint(x, pltpu.HBM)
        for x in (calcium, activation) + vectors
    ]
    edge, pair_weight, col_high, col_low = pl.pallas_call(
        edge_kernel,
        in_specs=[pl.BlockSpec(memory_space=pltpu.HBM)] * 8,
        out_shape=[
            jax.ShapeDtypeStruct((48, LANES), f32),
            jax.ShapeDtypeStruct((2 * ROWS, 1024), bf16),
            jax.ShapeDtypeStruct((512, 256), bf16),
            jax.ShapeDtypeStruct((512, 256), bf16),
        ],
        scratch_shapes=[line(x.shape[0], x.dtype) for x in vectors]
        + [
            pltpu.VMEM((2, 32, SUBS, 32, LANES), f32),
            pltpu.VMEM((32, 2048), f32),
            pltpu.SemaphoreType.DMA((6,)),
            pltpu.SemaphoreType.DMA((2, 32)),
        ],
        compiler_params=pltpu.CompilerParams(vmem_limit_bytes=16 << 20),
        name="edge",
    )(*far)
    incoming = lax.ppermute(edge, "gx", [(i, i + 1) for i in range(7)])
    field_spec = pl.BlockSpec((1, 32, 32, LANES), lambda s: (s, 0, 0, 0))
    flat = lambda *shape: pl.BlockSpec(shape, lambda s: (0, 0))
    blocks = pl.pallas_call(
        restrict_kernel,
        grid=(SUBS,),
        in_specs=[
            field_spec,
            field_spec,
            flat(2 * ROWS, 1024),
            flat(512, 256),
            flat(512, 256),
        ],
        out_specs=pl.BlockSpec((4, BLOCK, LANES), lambda s: (0, 0, 0)),
        out_shape=jax.ShapeDtypeStruct((4, BLOCK, LANES), f32),
        scratch_shapes=[
            pltpu.VMEM((4, 2 * ROWS, LANES), f32),
            pltpu.VMEM((2 * ROWS, 256), f32),
        ],
        compiler_params=pltpu.CompilerParams(
            dimension_semantics=("arbitrary",), vmem_limit_bytes=16 << 20
        ),
        name="restrict",
    )(calcium, activation, pair_weight, col_high, col_low)
    small = pltpu.CompilerParams(vmem_limit_bytes=4 << 20)
    message = jax.ShapeDtypeStruct((BLOCK, LANES), f32)
    messages = pl.pallas_call(route_kernel, out_shape=[message] * 4, compiler_params=small, name="route")(
        blocks, incoming
    )
    messages = exchange(messages, "gz")
    piece = jax.ShapeDtypeStruct((PIECE, LANES), f32)
    pieces = pl.pallas_call(
        combine_kernel,
        out_shape=[piece] * 4,
        scratch_shapes=[pltpu.VMEM((4, BLOCK, LANES), f32)],
        compiler_params=small,
        name="combine",
    )(*messages)
    pieces = exchange(pieces, "gy")
    result = jax.ShapeDtypeStruct(troponin.shape, f32)
    return pl.pallas_call(
        tension_kernel,
        out_shape=[result, result],
        scratch_shapes=[pltpu.VMEM((4, PIECE, LANES), f32)],
        compiler_params=small,
        name="tension",
    )(*pieces, troponin, tension, unbind_rate, relax_rate)


def solution(mesh):
    node_spec = P("gx", ("gy", "gz"), None)
    return jax.shard_map(
        per_device,
        mesh=mesh,
        in_specs=(P(None, "gx", "gz", "gy"),) * 2 + (P(),) * 6 + (node_spec,) * 4,
        out_specs=(node_spec, node_spec),
        check_vma=False,
    )
```

```python
import jax
import jax.numpy as jnp
from jax import lax
from jax.experimental import pallas as pl
from jax.experimental.pallas import tpu as pltpu
from jax.sharding import PartitionSpec as P

step_size = 0.2
bind_rate = 2.0
peak_tension = 2.0
half_square = 0.25

f32 = jnp.float32
bf16 = jnp.bfloat16
LANES = 128
SUBS = 8
NODES = 8
COLS = 32
ROWS = 72
BLOCK = 104
SURE = 28
PIECE = 72


def hat(element, offset, first_node, rows):
    cells = element.shape[0]
    element = element.reshape(1, cells)
    offset = offset.reshape(1, cells)
    node = first_node + lax.broadcasted_iota(jnp.int32, (rows, cells), 0)
    raw = jnp.where(element == node, 1.0 - offset, 0.0) + jnp.where(
        element + 1 == node, offset, 0.0
    )
    return raw / jnp.sum(raw, axis=1, keepdims=True)


def halves(value):
    high = value.astype(bf16).astype(f32)
    return high, value - high


def lane_ids(rows):
    return lax.broadcasted_iota(jnp.int32, (rows, LANES), 1)


def pick_lanes(values, index):
    return jnp.take_along_axis(values, index, axis=1, mode="promise_in_bounds")


def edge_kernel(
    calcium,
    activation,
    element_first,
    offset_first,
    element_second,
    offset_second,
    element_third,
    offset_third,
    edge,
    pair_weight,
    col_high,
    col_low,
    elements_1,
    offsets_1,
    elements_2,
    offsets_2,
    elements_3,
    offsets_3,
    cells,
    sums,
    small_sems,
    cell_sems,
):
    gx, gy, gz = lax.axis_index("gx"), lax.axis_index("gy"), lax.axis_index("gz")
    small = [
        (element_first, elements_1),
        (offset_first, offsets_1),
        (element_third, elements_3),
        (offset_third, offsets_3),
        (element_second, elements_2),
        (offset_second, offsets_2),
    ]
    loads = [
        pltpu.make_async_copy(source, target, small_sems.at[n])
        for n, (source, target) in enumerate(small)
    ]
    def cell_copies(x):
        return [
            pltpu.make_async_copy(field.at[:, x], cells.at[f, x], cell_sems.at[f, x])
            for f, field in enumerate((calcium, activation))
        ]

    for load in loads:
        load.start()
    for x in range(31, SURE - 1, -1):
        for copy in cell_copies(x):
            copy.start()
    loads[0].wait()

    place = lax.broadcasted_iota(jnp.int32, (1, 256), 1)
    earlier = jnp.logical_and(
        place // 32 == gx, elements_1[...].reshape(1, 256) < gx * NODES + NODES - 1
    )
    begin = jnp.sum(jnp.where(earlier, 1.0, 0.0)).astype(jnp.int32)

    def start(n, carry):
        for copy in cell_copies(SURE - 1 - n):
            copy.start()
        return carry

    lax.fori_loop(0, SURE - begin, start, 0)
    loads[1].wait()
    loads[2].wait()
    loads[3].wait()

    first = hat(elements_1[...], offsets_1[...], gx * NODES, 16)
    own = jnp.where(gx >= 4, first[:, LANES:], first[:, :LANES])
    third = hat(elements_3[...], offsets_3[...], gz * NODES, 16)
    lane = lane_ids(16)
    depth = pick_lanes(third, gz * 32 + lane % 32)
    for tile in range(8):
        row = pick_lanes(own, lax.rem(gx, 4) * 32 + 4 * tile + lane // 32)
        parts = [depth[b : b + 1] * row[:NODES] for b in range(NODES + 1)]
        both = jnp.concatenate(halves(jnp.concatenate(parts, 0)), 0)
        pair_weight[:, tile * LANES : (tile + 1) * LANES] = both.astype(bf16)

    loads[4].wait()
    loads[5].wait()
    second = hat(elements_2[...], offsets_2[...], gy * COLS, 40)
    chunk = second[:, :LANES]
    for c in range(1, 4):
        chunk = jnp.where(gy == c, second[:, c * LANES : (c + 1) * LANES], chunk)
    full = jnp.concatenate([chunk, jnp.zeros((LANES - 40, LANES), f32)], 0)
    turned = full.T
    lane = lane_ids(LANES)
    for group in range(4):
        first_lane = group * COLS
        main = turned if group == 0 else pltpu.roll(turned, first_lane, 1)
        main = jnp.where(lane // COLS == group, main, 0.0)
        shift = (first_lane - COLS) % LANES
        extra = turned if shift == 0 else pltpu.roll(turned, shift, 1)
        extra = jnp.where(lane == first_lane, extra, 0.0)
        high, low = halves(jnp.concatenate([main, extra], 1))
        rows = slice(group * LANES, (group + 1) * LANES)
        col_high[rows] = high.astype(bf16)
        col_low[rows] = low.astype(bf16)

    layer = jnp.broadcast_to(own[NODES : NODES + 1], (8, LANES))

    def cell_weight(x):
        index = jnp.full((8, LANES), lax.rem(gx, 4) * 32 + x, jnp.int32)
        return jnp.concatenate([pick_lanes(layer, index)] * 4, 0)

    slots = [(f, t, (f * SUBS + t) * LANES) for f in range(2) for t in range(SUBS)]
    sure = range(SURE, 32)
    for x in sure:
        for copy in cell_copies(x):
            copy.wait()
    sure_weights = [cell_weight(x) for x in sure]
    for f, t, column in slots:
        total = None
        for x, weight in zip(sure, sure_weights):
            part = weight * cells[f, x, t]
            total = part if total is None else total + part
        sums[:, column : column + LANES] = total

    def add(n, carry):
        x = SURE - 1 - n
        for copy in cell_copies(x):
            copy.wait()
        weight = cell_weight(x)
        for f, t, column in slots:
            sums[:, column : column + LANES] += weight * cells[f, x, t]
        return carry

    lax.fori_loop(0, SURE - begin, add, 0)

    depth_high, depth_low = halves(depth[:, :32])
    weights = jnp.concatenate([depth_high, depth_low], 0).astype(bf16)
    high, low = halves(sums[...])
    upper = jnp.dot(weights, high.astype(bf16), preferred_element_type=f32)
    lower = jnp.dot(weights[:16], low.astype(bf16), preferred_element_type=f32)
    planes = upper[:16] + upper[16:] + lower
    whole = jnp.concatenate([planes[:, j * 512 : (j + 1) * 512] for j in range(4)], 0)
    result = columns(whole, col_high, col_low)
    quads = [result[j * 16 : j * 16 + 16] for j in range(4)]
    extra = quads[0][:, LANES:]
    for j in range(1, 4):
        extra = extra + pltpu.roll(quads[j][:, LANES:], j, 1)
    for j in range(4):
        edge[j * 8 : j * 8 + 8] = quads[j][:8, :LANES]
    corners = [q[8:9, :LANES] for q in quads] + [extra[8:9]]
    edge[32:40] = jnp.concatenate(corners + [jnp.zeros((3, LANES), f32)], 0)
    edge[40:48] = extra[:8]


def columns(whole, col_high, col_low):
    high, low = halves(whole)
    high, low = high.astype(bf16), low.astype(bf16)
    return (
        jnp.dot(high, col_high[...], preferred_element_type=f32)
        + jnp.dot(low, col_high[...], preferred_element_type=f32)
        + jnp.dot(high, col_low[...], preferred_element_type=f32)
    )


def restrict_kernel(
    calcium, activation, pair_weight, col_high, col_low, blocks, partials, packed
):
    step = pl.program_id(0)
    cells = 32 * 32
    field = jnp.concatenate(
        [calcium[0].reshape(cells, LANES), activation[0].reshape(cells, LANES)], 1
    )
    high, low = halves(field)
    upper = jnp.dot(pair_weight[...], high.astype(bf16), preferred_element_type=f32)
    lower = jnp.dot(pair_weight[:80], low.astype(bf16), preferred_element_type=f32)
    section = upper[:ROWS] + upper[ROWS:] + lower[:ROWS]
    group = lax.rem(step, 4)
    partials[group, :ROWS] = section[:, :LANES]
    partials[group, ROWS:] = section[:, LANES:]

    def contract():
        whole = jnp.concatenate([partials[g] for g in range(4)], 1)
        return columns(whole, col_high, col_low)

    @pl.when(step == 3)
    def _():
        packed[...] = contract()

    @pl.when(step == SUBS - 1)
    def _():
        first, last = packed[...], contract()
        quads = [first[:ROWS], last[:ROWS], first[ROWS:], last[ROWS:]]
        main = [q[:, :LANES] for q in quads]
        extra = quads[0][:, LANES:]
        for j in range(1, 4):
            extra = extra + pltpu.roll(quads[j][:, LANES:], j, 1)
        for k in range(4):
            tail = None
            for p, plane in enumerate((2 * k, 2 * k + 1, NODES)):
                rows = slice(plane * 8, plane * 8 + 8)
                for j in range(4):
                    start = j * 24 + p * 8
                    blocks[k, start : start + 8] = main[j][rows]
                piece = extra[rows]
                piece = piece if p == 0 else pltpu.roll(piece, 4 * p, 1)
                tail = piece if tail is None else tail + piece
            blocks[k, 96:104] = tail


def route_kernel(blocks, incoming, *outs):
    gz = lax.axis_index("gz")
    top = lax.broadcasted_iota(jnp.int32, (8, LANES), 0) == 0
    for k in range(4):
        which = lax.rem(gz + k, 4)
        out = outs[k]
        tail = None
        for p in range(3):
            for j in range(4):
                start = j * 24 + p * 8
                if p < 2:
                    row = incoming[pl.ds(j * 8 + 2 * which + p, 1), :]
                else:
                    row = incoming[32 + j : 33 + j, :]
                out[start : start + 8] = blocks[which, start : start + 8] + jnp.where(
                    top, row, 0.0
                )
            if p < 2:
                row = incoming[pl.ds(40 + 2 * which + p, 1), :]
            else:
                row = incoming[36:37, :]
            row = jnp.where(top, row, 0.0)
            row = row if p == 0 else pltpu.roll(row, 4 * p, 1)
            tail = row if tail is None else tail + row
        out[96:104] = blocks[which, 96:104] + tail


def combine_kernel(own, one, two, three, *rest):
    outs, slabs = rest[:4], rest[4]
    gy, gz = lax.axis_index("gy"), lax.axis_index("gz")
    for k, message in enumerate((own, one, two, three)):
        slabs[lax.rem(gz + 4 - k, 4)] = message[...]
    lane = lane_ids(8)
    for k in range(4):
        slab = lax.rem(gy + k, 4)
        before = lax.rem(slab + 3, 4)
        joins = jnp.logical_and(gz == 0, slab > 0)
        out = outs[k]
        for j in range(4):
            start = j * 24
            plane = slabs[before, start + 16 : start + 24]
            out[j * 16 : j * 16 + 8] = slabs[slab, start : start + 8] + jnp.where(
                joins, plane, 0.0
            )
            out[j * 16 + 8 : j * 16 + 16] = slabs[slab, start + 8 : start + 16]
        tail = pltpu.roll(slabs[before, 96:104], LANES - 8, 1)
        tail = jnp.where(jnp.logical_and(joins, lane % COLS < 4), tail, 0.0)
        out[64:72] = slabs[slab, 96:104] + tail


def tension_kernel(
    own, one, two, three, troponin, tension, unbind, relax, bound_out, active_out, chunks
):
    gy = lax.axis_index("gy")
    for k, message in enumerate((own, one, two, three)):
        chunks[lax.rem(gy + 4 - k, 4)] = message[...]
    lane = lane_ids(8)
    pieces = [chunks[c] for c in range(4)]

    def turn(value, shift):
        shift = shift % LANES
        return value if shift == 0 else pltpu.roll(value, shift, 1)

    def drive(f, substep, plane):
        half, group = divmod(substep, 4)
        j = 2 * f + half
        start = j * 16 + plane * 8
        total = None
        for c in range(4):
            part = turn(pieces[c][start : start + 8], COLS * (c - group))
            total = part if total is None else jnp.where(lane // COLS == c, part, total)
        for c in range(3):
            shift = COLS * (c + 1) - (COLS * group + 4 * plane + j)
            part = turn(pieces[c][64:72], shift)
            total = total + jnp.where(lane == COLS * (c + 1), part, 0.0)
        return total

    for plane in range(2):
        bound = troponin[:, plane, :]
        active = tension[:, plane, :]
        unbinding = unbind[:, plane, :]
        relaxing = step_size * relax[:, plane, :]
        for substep in range(SUBS):
            calcium_now = drive(0, substep, plane)
            squared = calcium_now * calcium_now
            binding = squared / (squared + half_square)
            bound = bound + step_size * (
                bind_rate * binding * (1.0 - bound) - unbinding * bound
            )
            active = active + relaxing * (
                peak_tension * drive(1, substep, plane) * bound - active
            )
        bound_out[:, plane, :] = bound
        active_out[:, plane, :] = active


def exchange(messages, axis):
    received = [messages[0]]
    for k in range(1, 4):
        pairs = [(i, (i + k) % 4) for i in range(4)]
        received.append(lax.ppermute(messages[k], axis, pairs))
    return received


def per_device(
    calcium,
    activation,
    element_first,
    offset_first,
    element_second,
    offset_second,
    element_third,
    offset_third,
    troponin,
    tension,
    unbind_rate,
    relax_rate,
):
    line = lambda n, kind: pltpu.VMEM((n,), kind)
    vectors = (
        element_first,
        offset_first,
        element_second,
        offset_second,
        element_third,
        offset_third,
    )
    far = [
        pltpu.with_memory_space_constraint(x, pltpu.HBM)
        for x in (calcium, activation) + vectors
    ]
    edge, pair_weight, col_high, col_low = pl.pallas_call(
        edge_kernel,
        in_specs=[pl.BlockSpec(memory_space=pltpu.HBM)] * 8,
        out_shape=[
            jax.ShapeDtypeStruct((48, LANES), f32),
            jax.ShapeDtypeStruct((2 * ROWS, 1024), bf16),
            jax.ShapeDtypeStruct((512, 256), bf16),
            jax.ShapeDtypeStruct((512, 256), bf16),
        ],
        scratch_shapes=[line(x.shape[0], x.dtype) for x in vectors]
        + [
            pltpu.VMEM((2, 32, SUBS, 32, LANES), f32),
            pltpu.VMEM((32, 2048), f32),
            pltpu.SemaphoreType.DMA((6,)),
            pltpu.SemaphoreType.DMA((2, 32)),
        ],
        compiler_params=pltpu.CompilerParams(vmem_limit_bytes=16 << 20),
        name="edge",
    )(*far)
    incoming = lax.ppermute(edge, "gx", [(i, i + 1) for i in range(7)])
    field_spec = pl.BlockSpec((1, 32, 32, LANES), lambda s: (s, 0, 0, 0))
    flat = lambda *shape: pl.BlockSpec(shape, lambda s: (0, 0))
    blocks = pl.pallas_call(
        restrict_kernel,
        grid=(SUBS,),
        in_specs=[
            field_spec,
            field_spec,
            flat(2 * ROWS, 1024),
            flat(512, 256),
            flat(512, 256),
        ],
        out_specs=pl.BlockSpec((4, BLOCK, LANES), lambda s: (0, 0, 0)),
        out_shape=jax.ShapeDtypeStruct((4, BLOCK, LANES), f32),
        scratch_shapes=[
            pltpu.VMEM((4, 2 * ROWS, LANES), f32),
            pltpu.VMEM((2 * ROWS, 256), f32),
        ],
        compiler_params=pltpu.CompilerParams(
            dimension_semantics=("arbitrary",), vmem_limit_bytes=16 << 20
        ),
        name="restrict",
    )(calcium, activation, pair_weight, col_high, col_low)
    small = pltpu.CompilerParams(vmem_limit_bytes=4 << 20)
    message = jax.ShapeDtypeStruct((BLOCK, LANES), f32)
    messages = pl.pallas_call(route_kernel, out_shape=[message] * 4, compiler_params=small, name="route")(
        blocks, incoming
    )
    messages = exchange(messages, "gz")
    piece = jax.ShapeDtypeStruct((PIECE, LANES), f32)
    pieces = pl.pallas_call(
        combine_kernel,
        out_shape=[piece] * 4,
        scratch_shapes=[pltpu.VMEM((4, BLOCK, LANES), f32)],
        compiler_params=small,
        name="combine",
    )(*messages)
    pieces = exchange(pieces, "gy")
    result = jax.ShapeDtypeStruct(troponin.shape, f32)
    return pl.pallas_call(
        tension_kernel,
        out_shape=[result, result],
        scratch_shapes=[pltpu.VMEM((4, PIECE, LANES), f32)],
        compiler_params=small,
        name="tension",
    )(*pieces, troponin, tension, unbind_rate, relax_rate)


def solution(mesh):
    node_spec = P("gx", ("gy", "gz"), None)
    return jax.shard_map(
        per_device,
        mesh=mesh,
        in_specs=(P(None, "gx", "gz", "gy"),) * 2 + (P(),) * 6 + (node_spec,) * 4,
        out_specs=(node_spec, node_spec),
        check_vma=False,
    )
```

```python
import jax
import jax.numpy as jnp
from jax import lax
from jax.experimental import pallas as pl
from jax.experimental.pallas import tpu as pltpu
from jax.sharding import PartitionSpec as P

step_size = 0.2
bind_rate = 2.0
peak_tension = 2.0
half_square = 0.25

f32 = jnp.float32
bf16 = jnp.bfloat16
LANES = 128
SUBS = 8
NODES = 8
COLS = 32
ROWS = 72
BLOCK = 104
SURE = 28
PIECE = 72


def hat(element, offset, first_node, rows):
    cells = element.shape[0]
    element = element.reshape(1, cells)
    offset = offset.reshape(1, cells)
    node = first_node + lax.broadcasted_iota(jnp.int32, (rows, cells), 0)
    raw = jnp.where(element == node, 1.0 - offset, 0.0) + jnp.where(
        element + 1 == node, offset, 0.0
    )
    return raw / jnp.sum(raw, axis=1, keepdims=True)


def halves(value):
    high = value.astype(bf16).astype(f32)
    return high, value - high


def lane_ids(rows):
    return lax.broadcasted_iota(jnp.int32, (rows, LANES), 1)


def pick_lanes(values, index):
    return jnp.take_along_axis(values, index, axis=1, mode="promise_in_bounds")


def edge_kernel(
    calcium,
    activation,
    element_first,
    offset_first,
    element_second,
    offset_second,
    element_third,
    offset_third,
    edge,
    first_weight,
    depth_weight,
    col_high,
    col_low,
    elements_1,
    offsets_1,
    elements_2,
    offsets_2,
    elements_3,
    offsets_3,
    sure_cells,
    cells,
    sums,
    small_sems,
    sure_sem,
    cell_sems,
):
    gx, gy, gz = lax.axis_index("gx"), lax.axis_index("gy"), lax.axis_index("gz")
    small = [
        (element_first, elements_1),
        (offset_first, offsets_1),
        (element_third, elements_3),
        (offset_third, offsets_3),
        (element_second, elements_2),
        (offset_second, offsets_2),
    ]
    loads = [
        pltpu.make_async_copy(source, target, small_sems.at[n])
        for n, (source, target) in enumerate(small)
    ]
    fields = (calcium, activation)
    sure_copies = [
        pltpu.make_async_copy(field.at[:, SURE:], sure_cells.at[f], sure_sem)
        for f, field in enumerate(fields)
    ]
    for load in loads:
        load.start()
    for copy in sure_copies:
        copy.start()
    loads[0].wait()

    place = lax.broadcasted_iota(jnp.int32, (1, 256), 1)
    earlier = jnp.logical_and(
        place // 32 == gx, elements_1[...].reshape(1, 256) < gx * NODES + NODES - 1
    )
    begin = jnp.sum(jnp.where(earlier, 1.0, 0.0)).astype(jnp.int32)

    count = (SURE + 1 - begin) // 2

    def start(n, carry):
        for f, field in enumerate(fields):
            layers = pl.ds(SURE - 2 - 2 * n, 2)
            pltpu.make_async_copy(
                field.at[:, layers], cells.at[n, f], cell_sems.at[n]
            ).start()
        return carry

    lax.fori_loop(0, count, start, 0)
    loads[1].wait()
    loads[2].wait()
    loads[3].wait()

    first = hat(elements_1[...], offsets_1[...], gx * NODES, 16)
    own = jnp.where(gx >= 4, first[:, LANES:], first[:, :LANES])
    third = hat(elements_3[...], offsets_3[...], gz * NODES, 16)
    depth = pick_lanes(third, gz * 32 + lane_ids(16) % 32)
    first_weight[...] = own
    depth_weight[...] = depth

    loads[4].wait()
    loads[5].wait()
    second = hat(elements_2[...], offsets_2[...], gy * COLS, 40)
    chunk = second[:, :LANES]
    for c in range(1, 4):
        chunk = jnp.where(gy == c, second[:, c * LANES : (c + 1) * LANES], chunk)
    full = jnp.concatenate([chunk, jnp.zeros((LANES - 40, LANES), f32)], 0)
    turned = full.T
    lane = lane_ids(LANES)
    for group in range(4):
        first_lane = group * COLS
        main = turned if group == 0 else pltpu.roll(turned, first_lane, 1)
        main = jnp.where(lane // COLS == group, main, 0.0)
        shift = (first_lane - COLS) % LANES
        extra = turned if shift == 0 else pltpu.roll(turned, shift, 1)
        extra = jnp.where(lane == first_lane, extra, 0.0)
        high, low = halves(jnp.concatenate([main, extra], 1))
        rows = slice(group * LANES, (group + 1) * LANES)
        col_high[rows] = high.astype(bf16)
        col_low[rows] = low.astype(bf16)

    layer = jnp.broadcast_to(own[NODES : NODES + 1], (8, LANES))

    def cell_weight(x):
        index = jnp.full((8, LANES), lax.rem(gx, 4) * 32 + x, jnp.int32)
        return jnp.concatenate([pick_lanes(layer, index)] * 4, 0)

    slots = [(f, t, (f * SUBS + t) * LANES) for f in range(2) for t in range(SUBS)]
    pltpu.make_async_copy(sure_cells, sure_cells, sure_sem).wait()
    sure_weights = [cell_weight(x) for x in range(SURE, 32)]
    for f, t, column in slots:
        total = None
        for n, weight in enumerate(sure_weights):
            part = weight * sure_cells[f, t, n]
            total = part if total is None else total + part
        sums[:, column : column + LANES] = total

    def add(n, carry):
        pltpu.make_async_copy(cells.at[n], cells.at[n], cell_sems.at[n]).wait()
        pair = [cell_weight(SURE - 2 - 2 * n + i) for i in range(2)]
        for f, t, column in slots:
            part = pair[0] * cells[n, f, t, 0] + pair[1] * cells[n, f, t, 1]
            sums[:, column : column + LANES] += part
        return carry

    lax.fori_loop(0, count, add, 0)

    depth_high, depth_low = halves(depth[:, :32])
    weights = jnp.concatenate([depth_high, depth_low], 0).astype(bf16)
    high, low = halves(sums[...])
    upper = jnp.dot(weights, high.astype(bf16), preferred_element_type=f32)
    lower = jnp.dot(weights[:16], low.astype(bf16), preferred_element_type=f32)
    planes = upper[:16] + upper[16:] + lower
    whole = jnp.concatenate([planes[:, j * 512 : (j + 1) * 512] for j in range(4)], 0)
    result = columns(whole, col_high, col_low)
    quads = [result[j * 16 : j * 16 + 16] for j in range(4)]
    extra = quads[0][:, LANES:]
    for j in range(1, 4):
        extra = extra + pltpu.roll(quads[j][:, LANES:], j, 1)
    for j in range(4):
        edge[j * 8 : j * 8 + 8] = quads[j][:8, :LANES]
    corners = [q[8:9, :LANES] for q in quads] + [extra[8:9]]
    edge[32:40] = jnp.concatenate(corners + [jnp.zeros((3, LANES), f32)], 0)
    edge[40:48] = extra[:8]


def columns(whole, col_high, col_low):
    high, low = halves(whole)
    high, low = high.astype(bf16), low.astype(bf16)
    return (
        jnp.dot(high, col_high[...], preferred_element_type=f32)
        + jnp.dot(low, col_high[...], preferred_element_type=f32)
        + jnp.dot(high, col_low[...], preferred_element_type=f32)
    )


def restrict_kernel(
    calcium, activation, first_weight, depth_weight, col_high, col_low, blocks, pair_weight
):
    gx = lax.axis_index("gx")
    lane = lane_ids(16)
    own, depth = first_weight[...], depth_weight[...]
    for tile in range(8):
        row = pick_lanes(own, lax.rem(gx, 4) * 32 + 4 * tile + lane // 32)
        parts = [depth[b : b + 1] * row[:NODES] for b in range(NODES + 1)]
        both = jnp.concatenate(halves(jnp.concatenate(parts, 0)), 0)
        pair_weight[:, tile * LANES : (tile + 1) * LANES] = both.astype(bf16)

    cells = 32 * 32

    def section(t):
        field = jnp.concatenate(
            [calcium[t].reshape(cells, LANES), activation[t].reshape(cells, LANES)], 1
        )
        high, low = halves(field)
        upper = jnp.dot(pair_weight[...], high.astype(bf16), preferred_element_type=f32)
        lower = jnp.dot(pair_weight[:80], low.astype(bf16), preferred_element_type=f32)
        total = upper[:ROWS] + upper[ROWS:] + lower[:ROWS]
        return jnp.concatenate([total[:, :LANES], total[:, LANES:]], 0)

    packed = []
    for half in range(2):
        whole = jnp.concatenate([section(4 * half + g) for g in range(4)], 1)
        packed.append(columns(whole, col_high, col_low))
    quads = [packed[half][f * ROWS : (f + 1) * ROWS] for f in range(2) for half in range(2)]
    main = [q[:, :LANES] for q in quads]
    extra = quads[0][:, LANES:]
    for j in range(1, 4):
        extra = extra + pltpu.roll(quads[j][:, LANES:], j, 1)
    for k in range(4):
        tail = None
        for p, plane in enumerate((2 * k, 2 * k + 1, NODES)):
            rows = slice(plane * 8, plane * 8 + 8)
            for j in range(4):
                start = j * 24 + p * 8
                blocks[k, start : start + 8] = main[j][rows]
            piece = extra[rows]
            piece = piece if p == 0 else pltpu.roll(piece, 4 * p, 1)
            tail = piece if tail is None else tail + piece
        blocks[k, 96:104] = tail


def route_kernel(blocks, incoming, *outs):
    gz = lax.axis_index("gz")
    top = lax.broadcasted_iota(jnp.int32, (8, LANES), 0) == 0
    for k in range(4):
        which = lax.rem(gz + k, 4)
        out = outs[k]
        tail = None
        for p in range(3):
            for j in range(4):
                start = j * 24 + p * 8
                if p < 2:
                    row = incoming[pl.ds(j * 8 + 2 * which + p, 1), :]
                else:
                    row = incoming[32 + j : 33 + j, :]
                out[start : start + 8] = blocks[which, start : start + 8] + jnp.where(
                    top, row, 0.0
                )
            if p < 2:
                row = incoming[pl.ds(40 + 2 * which + p, 1), :]
            else:
                row = incoming[36:37, :]
            row = jnp.where(top, row, 0.0)
            row = row if p == 0 else pltpu.roll(row, 4 * p, 1)
            tail = row if tail is None else tail + row
        out[96:104] = blocks[which, 96:104] + tail


def combine_kernel(own, one, two, three, *rest):
    outs, slabs = rest[:4], rest[4]
    gy, gz = lax.axis_index("gy"), lax.axis_index("gz")
    for k, message in enumerate((own, one, two, three)):
        slabs[lax.rem(gz + 4 - k, 4)] = message[...]
    lane = lane_ids(8)
    for k in range(4):
        slab = lax.rem(gy + k, 4)
        before = lax.rem(slab + 3, 4)
        joins = jnp.logical_and(gz == 0, slab > 0)
        out = outs[k]
        for j in range(4):
            start = j * 24
            plane = slabs[before, start + 16 : start + 24]
            out[j * 16 : j * 16 + 8] = slabs[slab, start : start + 8] + jnp.where(
                joins, plane, 0.0
            )
            out[j * 16 + 8 : j * 16 + 16] = slabs[slab, start + 8 : start + 16]
        tail = pltpu.roll(slabs[before, 96:104], LANES - 8, 1)
        tail = jnp.where(jnp.logical_and(joins, lane % COLS < 4), tail, 0.0)
        out[64:72] = slabs[slab, 96:104] + tail


def tension_kernel(
    own, one, two, three, troponin, tension, unbind, relax, bound_out, active_out, chunks
):
    gy = lax.axis_index("gy")
    for k, message in enumerate((own, one, two, three)):
        chunks[lax.rem(gy + 4 - k, 4)] = message[...]
    lane = lane_ids(8)
    pieces = [chunks[c] for c in range(4)]

    def turn(value, shift):
        shift = shift % LANES
        return value if shift == 0 else pltpu.roll(value, shift, 1)

    def drive(f, substep, plane):
        half, group = divmod(substep, 4)
        j = 2 * f + half
        start = j * 16 + plane * 8
        total = None
        for c in range(4):
            part = turn(pieces[c][start : start + 8], COLS * (c - group))
            total = part if total is None else jnp.where(lane // COLS == c, part, total)
        for c in range(3):
            shift = COLS * (c + 1) - (COLS * group + 4 * plane + j)
            part = turn(pieces[c][64:72], shift)
            total = total + jnp.where(lane == COLS * (c + 1), part, 0.0)
        return total

    for plane in range(2):
        bound = troponin[:, plane, :]
        active = tension[:, plane, :]
        unbinding = unbind[:, plane, :]
        relaxing = step_size * relax[:, plane, :]
        for substep in range(SUBS):
            calcium_now = drive(0, substep, plane)
            squared = calcium_now * calcium_now
            binding = squared / (squared + half_square)
            bound = bound + step_size * (
                bind_rate * binding * (1.0 - bound) - unbinding * bound
            )
            active = active + relaxing * (
                peak_tension * drive(1, substep, plane) * bound - active
            )
        bound_out[:, plane, :] = bound
        active_out[:, plane, :] = active


def exchange(messages, axis):
    received = [messages[0]]
    for k in range(1, 4):
        pairs = [(i, (i + k) % 4) for i in range(4)]
        received.append(lax.ppermute(messages[k], axis, pairs))
    return received


def per_device(
    calcium,
    activation,
    element_first,
    offset_first,
    element_second,
    offset_second,
    element_third,
    offset_third,
    troponin,
    tension,
    unbind_rate,
    relax_rate,
):
    line = lambda n, kind: pltpu.VMEM((n,), kind)
    vectors = (
        element_first,
        offset_first,
        element_second,
        offset_second,
        element_third,
        offset_third,
    )
    far = [
        pltpu.with_memory_space_constraint(x, pltpu.HBM)
        for x in (calcium, activation) + vectors
    ]
    edge, *weights = pl.pallas_call(
        edge_kernel,
        in_specs=[pl.BlockSpec(memory_space=pltpu.HBM)] * 8,
        out_shape=[
            jax.ShapeDtypeStruct((48, LANES), f32),
            jax.ShapeDtypeStruct((16, LANES), f32),
            jax.ShapeDtypeStruct((16, LANES), f32),
            jax.ShapeDtypeStruct((512, 256), bf16),
            jax.ShapeDtypeStruct((512, 256), bf16),
        ],
        scratch_shapes=[line(x.shape[0], x.dtype) for x in vectors]
        + [
            pltpu.VMEM((2, SUBS, 32 - SURE, 32, LANES), f32),
            pltpu.VMEM((SURE // 2, 2, SUBS, 2, 32, LANES), f32),
            pltpu.VMEM((32, 2048), f32),
            pltpu.SemaphoreType.DMA((6,)),
            pltpu.SemaphoreType.DMA,
            pltpu.SemaphoreType.DMA((SURE // 2,)),
        ],
        compiler_params=pltpu.CompilerParams(vmem_limit_bytes=16 << 20),
        name="edge",
    )(*far)
    incoming = lax.ppermute(edge, "gx", [(i, i + 1) for i in range(7)])
    blocks = pl.pallas_call(
        restrict_kernel,
        out_shape=jax.ShapeDtypeStruct((4, BLOCK, LANES), f32),
        scratch_shapes=[pltpu.VMEM((2 * ROWS, 1024), bf16)],
        compiler_params=pltpu.CompilerParams(vmem_limit_bytes=16 << 20),
        name="restrict",
    )(calcium, activation, *weights)
    small = pltpu.CompilerParams(vmem_limit_bytes=4 << 20)
    message = jax.ShapeDtypeStruct((BLOCK, LANES), f32)
    messages = pl.pallas_call(route_kernel, out_shape=[message] * 4, compiler_params=small, name="route")(
        blocks, incoming
    )
    messages = exchange(messages, "gz")
    piece = jax.ShapeDtypeStruct((PIECE, LANES), f32)
    pieces = pl.pallas_call(
        combine_kernel,
        out_shape=[piece] * 4,
        scratch_shapes=[pltpu.VMEM((4, BLOCK, LANES), f32)],
        compiler_params=small,
        name="combine",
    )(*messages)
    pieces = exchange(pieces, "gy")
    result = jax.ShapeDtypeStruct(troponin.shape, f32)
    return pl.pallas_call(
        tension_kernel,
        out_shape=[result, result],
        scratch_shapes=[pltpu.VMEM((4, PIECE, LANES), f32)],
        compiler_params=small,
        name="tension",
    )(*pieces, troponin, tension, unbind_rate, relax_rate)


def solution(mesh):
    node_spec = P("gx", ("gy", "gz"), None)
    return jax.shard_map(
        per_device,
        mesh=mesh,
        in_specs=(P(None, "gx", "gz", "gy"),) * 2 + (P(),) * 6 + (node_spec,) * 4,
        out_specs=(node_spec, node_spec),
        check_vma=False,
    )
```

```python
import jax
import jax.numpy as jnp
from jax import lax
from jax.experimental import pallas as pl
from jax.experimental.pallas import tpu as pltpu
from jax.sharding import PartitionSpec as P


step_size = 0.2
bind_rate = 2.0
peak_tension = 2.0
half_square = 0.25

f32 = jnp.float32
bf16 = jnp.bfloat16
LANES = 128
SUBS = 8
NODES = 8
COLS = 32
ROWS = 72
BLOCK = 104
SURE = 28
PIECE = 72


def hat(element, offset, first_node, rows):
    cells = element.shape[0]
    element = element.reshape(1, cells)
    offset = offset.reshape(1, cells)
    node = first_node + lax.broadcasted_iota(jnp.int32, (rows, cells), 0)
    raw = jnp.where(element == node, 1.0 - offset, 0.0) + jnp.where(
        element + 1 == node, offset, 0.0
    )
    return raw / jnp.sum(raw, axis=1, keepdims=True)


def halves(value):
    high = value.astype(bf16).astype(f32)
    return high, value - high


def lane_ids(rows):
    return lax.broadcasted_iota(jnp.int32, (rows, LANES), 1)


def pick_lanes(values, index):
    return jnp.take_along_axis(values, index, axis=1, mode="promise_in_bounds")


def edge_kernel(
    calcium,
    activation,
    element_first,
    offset_first,
    element_second,
    offset_second,
    element_third,
    offset_third,
    edge,
    first_weight,
    depth_weight,
    col_high,
    col_low,
    elements_1,
    offsets_1,
    elements_2,
    offsets_2,
    elements_3,
    offsets_3,
    sure_cells,
    cells,
    sums,
    small_sems,
    sure_sem,
    cell_sems,
):
    gx, gy, gz = lax.axis_index("gx"), lax.axis_index("gy"), lax.axis_index("gz")
    small = [
        (element_first, elements_1),
        (offset_first, offsets_1),
        (element_third, elements_3),
        (offset_third, offsets_3),
        (element_second, elements_2),
        (offset_second, offsets_2),
    ]
    loads = [
        pltpu.make_async_copy(source, target, small_sems.at[n])
        for n, (source, target) in enumerate(small)
    ]
    fields = (calcium, activation)
    sure_copies = [
        pltpu.make_async_copy(field.at[:, SURE:], sure_cells.at[f], sure_sem)
        for f, field in enumerate(fields)
    ]
    for load in loads:
        load.start()
    for copy in sure_copies:
        copy.start()
    loads[0].wait()

    place = lax.broadcasted_iota(jnp.int32, (1, 256), 1)
    earlier = jnp.logical_and(
        place // 32 == gx, elements_1[...].reshape(1, 256) < gx * NODES + NODES - 1
    )
    begin = jnp.sum(jnp.where(earlier, 1.0, 0.0)).astype(jnp.int32)

    count = (SURE + 1 - begin) // 2

    def start(n, carry):
        for f, field in enumerate(fields):
            layers = pl.ds(SURE - 2 - 2 * n, 2)
            pltpu.make_async_copy(
                field.at[:, layers], cells.at[n, f], cell_sems.at[n]
            ).start()
        return carry

    lax.fori_loop(0, count, start, 0)
    loads[1].wait()
    loads[2].wait()
    loads[3].wait()

    first = hat(elements_1[...], offsets_1[...], gx * NODES, 16)
    own = jnp.where(gx >= 4, first[:, LANES:], first[:, :LANES])
    third = hat(elements_3[...], offsets_3[...], gz * NODES, 16)
    depth = pick_lanes(third, gz * 32 + lane_ids(16) % 32)
    first_weight[...] = own
    depth_weight[...] = depth

    loads[4].wait()
    loads[5].wait()
    second = hat(elements_2[...], offsets_2[...], gy * COLS, 40)
    chunk = second[:, :LANES]
    for c in range(1, 4):
        chunk = jnp.where(gy == c, second[:, c * LANES : (c + 1) * LANES], chunk)
    full = jnp.concatenate([chunk, jnp.zeros((LANES - 40, LANES), f32)], 0)
    turned = full.T
    lane = lane_ids(LANES)
    for group in range(4):
        first_lane = group * COLS
        main = turned if group == 0 else pltpu.roll(turned, first_lane, 1)
        main = jnp.where(lane // COLS == group, main, 0.0)
        shift = (first_lane - COLS) % LANES
        extra = turned if shift == 0 else pltpu.roll(turned, shift, 1)
        extra = jnp.where(lane == first_lane, extra, 0.0)
        high, low = halves(jnp.concatenate([main, extra], 1))
        rows = slice(group * LANES, (group + 1) * LANES)
        col_high[rows] = high.astype(bf16)
        col_low[rows] = low.astype(bf16)

    layer = jnp.broadcast_to(own[NODES : NODES + 1], (8, LANES))

    def cell_weight(x):
        index = jnp.full((8, LANES), lax.rem(gx, 4) * 32 + x, jnp.int32)
        return jnp.concatenate([pick_lanes(layer, index)] * 4, 0)

    slots = [(f, t, (f * SUBS + t) * LANES) for f in range(2) for t in range(SUBS)]
    pltpu.make_async_copy(sure_cells, sure_cells, sure_sem).wait()
    sure_weights = [cell_weight(x) for x in range(SURE, 32)]
    for f, t, column in slots:
        total = None
        for n, weight in enumerate(sure_weights):
            part = weight * sure_cells[f, t, n]
            total = part if total is None else total + part
        sums[:, column : column + LANES] = total

    def add(n, carry):
        pltpu.make_async_copy(cells.at[n], cells.at[n], cell_sems.at[n]).wait()
        pair = [cell_weight(SURE - 2 - 2 * n + i) for i in range(2)]
        for f, t, column in slots:
            part = pair[0] * cells[n, f, t, 0] + pair[1] * cells[n, f, t, 1]
            sums[:, column : column + LANES] += part
        return carry

    lax.fori_loop(0, count, add, 0)

    depth_high, depth_low = halves(depth[:, :32])
    weights = jnp.concatenate([depth_high, depth_low], 0).astype(bf16)
    high, low = halves(sums[...])
    upper = jnp.dot(weights, high.astype(bf16), preferred_element_type=f32)
    lower = jnp.dot(weights[:16], low.astype(bf16), preferred_element_type=f32)
    planes = upper[:16] + upper[16:] + lower
    whole = jnp.concatenate([planes[:, j * 512 : (j + 1) * 512] for j in range(4)], 0)
    result = columns(whole, col_high, col_low)
    quads = [result[j * 16 : j * 16 + 16] for j in range(4)]
    extra = quads[0][:, LANES:]
    for j in range(1, 4):
        extra = extra + pltpu.roll(quads[j][:, LANES:], j, 1)
    for j in range(4):
        edge[j * 8 : j * 8 + 8] = quads[j][:8, :LANES]
    corners = [q[8:9, :LANES] for q in quads] + [extra[8:9]]
    edge[32:40] = jnp.concatenate(corners + [jnp.zeros((3, LANES), f32)], 0)
    edge[40:48] = extra[:8]


def columns(whole, col_high, col_low):
    high, low = halves(whole)
    high, low = high.astype(bf16), low.astype(bf16)
    return (
        jnp.dot(high, col_high[...], preferred_element_type=f32)
        + jnp.dot(low, col_high[...], preferred_element_type=f32)
        + jnp.dot(high, col_low[...], preferred_element_type=f32)
    )


def restrict_kernel(
    calcium, activation, first_weight, depth_weight, col_high, col_low, blocks, pair_weight
):
    gx = lax.axis_index("gx")
    lane = lane_ids(16)
    own, depth = first_weight[...], depth_weight[...]
    for tile in range(8):
        row = pick_lanes(own, lax.rem(gx, 4) * 32 + 4 * tile + lane // 32)
        parts = [depth[b : b + 1] * row[:NODES] for b in range(NODES + 1)]
        both = jnp.concatenate(halves(jnp.concatenate(parts, 0)), 0)
        pair_weight[:, tile * LANES : (tile + 1) * LANES] = both.astype(bf16)

    cells = 32 * 32

    def section(t):
        field = jnp.concatenate(
            [calcium[t].reshape(cells, LANES), activation[t].reshape(cells, LANES)], 1
        )
        high, low = halves(field)
        upper = jnp.dot(pair_weight[...], high.astype(bf16), preferred_element_type=f32)
        lower = jnp.dot(pair_weight[:80], low.astype(bf16), preferred_element_type=f32)
        total = upper[:ROWS] + upper[ROWS:] + lower[:ROWS]
        return jnp.concatenate([total[:, :LANES], total[:, LANES:]], 0)

    packed = []
    for half in range(2):
        whole = jnp.concatenate([section(4 * half + g) for g in range(4)], 1)
        packed.append(columns(whole, col_high, col_low))
    quads = [packed[half][f * ROWS : (f + 1) * ROWS] for f in range(2) for half in range(2)]
    main = [q[:, :LANES] for q in quads]
    extra = quads[0][:, LANES:]
    for j in range(1, 4):
        extra = extra + pltpu.roll(quads[j][:, LANES:], j, 1)
    for k in range(4):
        tail = None
        for p, plane in enumerate((2 * k, 2 * k + 1, NODES)):
            rows = slice(plane * 8, plane * 8 + 8)
            for j in range(4):
                start = j * 24 + p * 8
                blocks[k, start : start + 8] = main[j][rows]
            piece = extra[rows]
            piece = piece if p == 0 else pltpu.roll(piece, 4 * p, 1)
            tail = piece if tail is None else tail + piece
        blocks[k, 96:104] = tail


def route_kernel(blocks, incoming, *outs):
    gz = lax.axis_index("gz")
    top = lax.broadcasted_iota(jnp.int32, (8, LANES), 0) == 0
    top = jnp.logical_and(top, lax.axis_index("gx") > 0)
    for k in range(4):
        which = lax.rem(gz + k, 4)
        out = outs[k]
        tail = None
        for p in range(3):
            for j in range(4):
                start = j * 24 + p * 8
                if p < 2:
                    row = incoming[pl.ds(j * 8 + 2 * which + p, 1), :]
                else:
                    row = incoming[32 + j : 33 + j, :]
                out[start : start + 8] = blocks[which, start : start + 8] + jnp.where(
                    top, row, 0.0
                )
            if p < 2:
                row = incoming[pl.ds(40 + 2 * which + p, 1), :]
            else:
                row = incoming[36:37, :]
            row = jnp.where(top, row, 0.0)
            row = row if p == 0 else pltpu.roll(row, 4 * p, 1)
            tail = row if tail is None else tail + row
        out[96:104] = blocks[which, 96:104] + tail


def combine_kernel(own, one, two, three, *rest):
    outs, slabs = rest[:4], rest[4]
    gy, gz = lax.axis_index("gy"), lax.axis_index("gz")
    for k, message in enumerate((own, one, two, three)):
        slabs[lax.rem(gz + 4 - k, 4)] = message[...]
    lane = lane_ids(8)
    for k in range(4):
        slab = lax.rem(gy + k, 4)
        before = lax.rem(slab + 3, 4)
        joins = jnp.logical_and(gz == 0, slab > 0)
        out = outs[k]
        for j in range(4):
            start = j * 24
            plane = slabs[before, start + 16 : start + 24]
            out[j * 16 : j * 16 + 8] = slabs[slab, start : start + 8] + jnp.where(
                joins, plane, 0.0
            )
            out[j * 16 + 8 : j * 16 + 16] = slabs[slab, start + 8 : start + 16]
        tail = pltpu.roll(slabs[before, 96:104], LANES - 8, 1)
        tail = jnp.where(jnp.logical_and(joins, lane % COLS < 4), tail, 0.0)
        out[64:72] = slabs[slab, 96:104] + tail


def tension_kernel(
    own, one, two, three, troponin, tension, unbind, relax, bound_out, active_out, chunks
):
    gy = lax.axis_index("gy")
    for k, message in enumerate((own, one, two, three)):
        chunks[lax.rem(gy + 4 - k, 4)] = message[...]
    lane = lane_ids(8)
    pieces = [chunks[c] for c in range(4)]

    def turn(value, shift):
        shift = shift % LANES
        return value if shift == 0 else pltpu.roll(value, shift, 1)

    def drive(f, substep, plane):
        half, group = divmod(substep, 4)
        j = 2 * f + half
        start = j * 16 + plane * 8
        total = None
        for c in range(4):
            part = turn(pieces[c][start : start + 8], COLS * (c - group))
            total = part if total is None else jnp.where(lane // COLS == c, part, total)
        for c in range(3):
            shift = COLS * (c + 1) - (COLS * group + 4 * plane + j)
            part = turn(pieces[c][64:72], shift)
            total = total + jnp.where(lane == COLS * (c + 1), part, 0.0)
        return total

    for plane in range(2):
        bound = troponin[:, plane, :]
        active = tension[:, plane, :]
        unbinding = unbind[:, plane, :]
        relaxing = step_size * relax[:, plane, :]
        for substep in range(SUBS):
            calcium_now = drive(0, substep, plane)
            squared = calcium_now * calcium_now
            binding = squared / (squared + half_square)
            bound = bound + step_size * (
                bind_rate * binding * (1.0 - bound) - unbinding * bound
            )
            active = active + relaxing * (
                peak_tension * drive(1, substep, plane) * bound - active
            )
        bound_out[:, plane, :] = bound
        active_out[:, plane, :] = active


def exchange(messages, axis):
    received = [messages[0]] + [None] * 3
    for k in range(1, 4):
        pairs = [(i, (i + k) % 4) for i in range(4)]
        received[k] = lax.ppermute(messages[k], axis, pairs)
    return received


def per_device(
    calcium,
    activation,
    element_first,
    offset_first,
    element_second,
    offset_second,
    element_third,
    offset_third,
    troponin,
    tension,
    unbind_rate,
    relax_rate,
):
    line = lambda n, kind: pltpu.VMEM((n,), kind)
    vectors = (
        element_first,
        offset_first,
        element_second,
        offset_second,
        element_third,
        offset_third,
    )
    far = [
        pltpu.with_memory_space_constraint(x, pltpu.HBM)
        for x in (calcium, activation) + vectors
    ]
    edge, *weights = pl.pallas_call(
        edge_kernel,
        in_specs=[pl.BlockSpec(memory_space=pltpu.HBM)] * 8,
        out_shape=[
            jax.ShapeDtypeStruct((48, LANES), f32),
            jax.ShapeDtypeStruct((16, LANES), f32),
            jax.ShapeDtypeStruct((16, LANES), f32),
            jax.ShapeDtypeStruct((512, 256), bf16),
            jax.ShapeDtypeStruct((512, 256), bf16),
        ],
        scratch_shapes=[line(x.shape[0], x.dtype) for x in vectors]
        + [
            pltpu.VMEM((2, SUBS, 32 - SURE, 32, LANES), f32),
            pltpu.VMEM((SURE // 2, 2, SUBS, 2, 32, LANES), f32),
            pltpu.VMEM((32, 2048), f32),
            pltpu.SemaphoreType.DMA((6,)),
            pltpu.SemaphoreType.DMA,
            pltpu.SemaphoreType.DMA((SURE // 2,)),
        ],
        compiler_params=pltpu.CompilerParams(vmem_limit_bytes=16 << 20),
        name="edge",
    )(*far)
    incoming = lax.ppermute(edge, "gx", [(i, (i + 1) % 8) for i in range(8)])
    blocks = pl.pallas_call(
        restrict_kernel,
        out_shape=jax.ShapeDtypeStruct((4, BLOCK, LANES), f32),
        scratch_shapes=[pltpu.VMEM((2 * ROWS, 1024), bf16)],
        compiler_params=pltpu.CompilerParams(vmem_limit_bytes=16 << 20),
        name="restrict",
    )(calcium, activation, *weights)
    small = pltpu.CompilerParams(vmem_limit_bytes=4 << 20)
    message = jax.ShapeDtypeStruct((BLOCK, LANES), f32)
    messages = pl.pallas_call(route_kernel, out_shape=[message] * 4, compiler_params=small, name="route")(
        blocks, incoming
    )
    messages = exchange(messages, "gz")
    piece = jax.ShapeDtypeStruct((PIECE, LANES), f32)
    pieces = pl.pallas_call(
        combine_kernel,
        out_shape=[piece] * 4,
        scratch_shapes=[pltpu.VMEM((4, BLOCK, LANES), f32)],
        compiler_params=small,
        name="combine",
    )(*messages)
    pieces = exchange(pieces, "gy")
    result = jax.ShapeDtypeStruct(troponin.shape, f32)
    return pl.pallas_call(
        tension_kernel,
        out_shape=[result, result],
        scratch_shapes=[pltpu.VMEM((4, PIECE, LANES), f32)],
        compiler_params=small,
        name="tension",
    )(*pieces, troponin, tension, unbind_rate, relax_rate)


def solution(mesh):
    node_spec = P("gx", ("gy", "gz"), None)
    return jax.shard_map(
        per_device,
        mesh=mesh,
        in_specs=(P(None, "gx", "gz", "gy"),) * 2 + (P(),) * 6 + (node_spec,) * 4,
        out_specs=(node_spec, node_spec),
        check_vma=False,
    )
```

```python
import jax
import jax.numpy as jnp
from jax import lax
from jax.experimental import pallas as pl
from jax.experimental.pallas import tpu as pltpu
from jax.sharding import PartitionSpec as P


step_size = 0.2
bind_rate = 2.0
peak_tension = 2.0
half_square = 0.25

f32 = jnp.float32
bf16 = jnp.bfloat16
LANES = 128
SUBS = 8
NODES = 8
COLS = 32
ROWS = 72
BLOCK = 104
SURE = 26
PIECE = 72


def hat(element, offset, first_node, rows):
    cells = element.shape[0]
    element = element.reshape(1, cells)
    offset = offset.reshape(1, cells)
    node = first_node + lax.broadcasted_iota(jnp.int32, (rows, cells), 0)
    raw = jnp.where(element == node, 1.0 - offset, 0.0) + jnp.where(
        element + 1 == node, offset, 0.0
    )
    return raw / jnp.sum(raw, axis=1, keepdims=True)


def halves(value):
    high = value.astype(bf16).astype(f32)
    return high, value - high


def plane_row(j, p):
    return j * 16 + p * 8 if p < 2 else PIECE + j * 8


def lane_ids(rows):
    return lax.broadcasted_iota(jnp.int32, (rows, LANES), 1)


def pick_lanes(values, index):
    return jnp.take_along_axis(values, index, axis=1, mode="promise_in_bounds")


def edge_kernel(
    calcium,
    activation,
    element_first,
    offset_first,
    element_second,
    offset_second,
    element_third,
    offset_third,
    edge,
    first_weight,
    depth_weight,
    col_high,
    col_low,
    elements_1,
    offsets_1,
    elements_2,
    offsets_2,
    elements_3,
    offsets_3,
    sure_cells,
    cells,
    sums,
    small_sems,
    sure_sem,
    cell_sems,
):
    gx, gy, gz = lax.axis_index("gx"), lax.axis_index("gy"), lax.axis_index("gz")
    small = [
        (element_first, elements_1),
        (offset_first, offsets_1),
        (element_third, elements_3),
        (offset_third, offsets_3),
        (element_second, elements_2),
        (offset_second, offsets_2),
    ]
    loads = [
        pltpu.make_async_copy(source, target, small_sems.at[n])
        for n, (source, target) in enumerate(small)
    ]
    fields = (calcium, activation)
    sure_copies = [
        pltpu.make_async_copy(field.at[:, SURE:], sure_cells.at[f], sure_sem)
        for f, field in enumerate(fields)
    ]
    for load in loads:
        load.start()
    for copy in sure_copies:
        copy.start()
    for load in loads[:4]:
        load.wait()

    first = hat(elements_1[...], offsets_1[...], gx * NODES, 16)
    own = jnp.where(gx >= 4, first[:, LANES:], first[:, :LANES])
    third = hat(elements_3[...], offsets_3[...], gz * NODES, 16)
    depth = pick_lanes(third, gz * 32 + lane_ids(16) % 32)
    first_weight[...] = own
    depth_weight[...] = depth

    place = lax.broadcasted_iota(jnp.int32, (1, 256), 1)
    earlier = jnp.logical_and(
        place // 32 == gx, elements_1[...].reshape(1, 256) < gx * NODES + NODES - 1
    )
    begin = jnp.sum(jnp.where(earlier, 1.0, 0.0)).astype(jnp.int32)

    count = (SURE + 1 - begin) // 2

    def start(n, carry):
        for f, field in enumerate(fields):
            layers = pl.ds(SURE - 2 - 2 * n, 2)
            pltpu.make_async_copy(
                field.at[:, layers], cells.at[n, f], cell_sems.at[n]
            ).start()
        return carry

    lax.fori_loop(0, count, start, 0)
    loads[4].wait()
    loads[5].wait()
    second = hat(elements_2[...], offsets_2[...], gy * COLS, 40)
    chunk = second[:, :LANES]
    for c in range(1, 4):
        chunk = jnp.where(gy == c, second[:, c * LANES : (c + 1) * LANES], chunk)
    full = jnp.concatenate([chunk, jnp.zeros((LANES - 40, LANES), f32)], 0)
    turned = full.T
    lane = lane_ids(LANES)
    for group in range(4):
        first_lane = group * COLS
        main = turned if group == 0 else pltpu.roll(turned, first_lane, 1)
        main = jnp.where(lane // COLS == group, main, 0.0)
        shift = (first_lane - COLS) % LANES
        extra = turned if shift == 0 else pltpu.roll(turned, shift, 1)
        extra = jnp.where(lane == first_lane, extra, 0.0)
        high, low = halves(jnp.concatenate([main, extra], 1))
        rows = slice(group * LANES, (group + 1) * LANES)
        col_high[rows] = high.astype(bf16)
        col_low[rows] = low.astype(bf16)

    layer = jnp.broadcast_to(own[NODES : NODES + 1], (8, LANES))

    def cell_weight(x):
        index = jnp.full((8, LANES), lax.rem(gx, 4) * 32 + x, jnp.int32)
        return jnp.concatenate([pick_lanes(layer, index)] * 4, 0)

    slots = [(f, t, (f * SUBS + t) * LANES) for f in range(2) for t in range(SUBS)]
    pltpu.make_async_copy(sure_cells, sure_cells, sure_sem).wait()
    sure_weights = [cell_weight(x) for x in range(SURE, 32)]
    for f, t, column in slots:
        total = None
        for n, weight in enumerate(sure_weights):
            part = weight * sure_cells[f, t, n]
            total = part if total is None else total + part
        sums[:, column : column + LANES] = total

    def add(n, carry):
        pltpu.make_async_copy(cells.at[n], cells.at[n], cell_sems.at[n]).wait()
        pair = [cell_weight(SURE - 2 - 2 * n + i) for i in range(2)]
        for f, t, column in slots:
            part = pair[0] * cells[n, f, t, 0] + pair[1] * cells[n, f, t, 1]
            sums[:, column : column + LANES] += part
        return carry

    lax.fori_loop(0, count, add, 0)

    depth_high, depth_low = halves(depth[:, :32])
    weights = jnp.concatenate([depth_high, depth_low], 0).astype(bf16)
    high, low = halves(sums[...])
    upper = jnp.dot(weights, high.astype(bf16), preferred_element_type=f32)
    lower = jnp.dot(weights[:16], low.astype(bf16), preferred_element_type=f32)
    planes = upper[:16] + upper[16:] + lower
    whole = jnp.concatenate([planes[:, j * 512 : (j + 1) * 512] for j in range(4)], 0)
    result = columns(whole, col_high, col_low)
    quads = [result[j * 16 : j * 16 + 16] for j in range(4)]
    extra = quads[0][:, LANES:]
    for j in range(1, 4):
        extra = extra + pltpu.roll(quads[j][:, LANES:], j, 1)
    for j in range(4):
        edge[j * 8 : j * 8 + 8] = quads[j][:8, :LANES]
    corners = [q[8:9, :LANES] for q in quads] + [extra[8:9]]
    edge[32:40] = jnp.concatenate(corners + [jnp.zeros((3, LANES), f32)], 0)
    edge[40:48] = extra[:8]


def columns(whole, col_high, col_low):
    high, low = halves(whole)
    high, low = high.astype(bf16), low.astype(bf16)
    return (
        jnp.dot(high, col_high[...], preferred_element_type=f32)
        + jnp.dot(low, col_high[...], preferred_element_type=f32)
        + jnp.dot(high, col_low[...], preferred_element_type=f32)
    )


def restrict_kernel(
    calcium, activation, first_weight, depth_weight, col_high, col_low, blocks, pair_weight
):
    gx = lax.axis_index("gx")
    lane = lane_ids(16)
    own, depth = first_weight[...], depth_weight[...]
    for tile in range(8):
        row = pick_lanes(own, lax.rem(gx, 4) * 32 + 4 * tile + lane // 32)
        parts = [depth[b : b + 1] * row[:NODES] for b in range(NODES + 1)]
        both = jnp.concatenate(halves(jnp.concatenate(parts, 0)), 0)
        pair_weight[:, tile * LANES : (tile + 1) * LANES] = both.astype(bf16)

    cells = 32 * 32

    def section(t):
        field = jnp.concatenate(
            [calcium[t].reshape(cells, LANES), activation[t].reshape(cells, LANES)], 1
        )
        high, low = halves(field)
        upper = jnp.dot(pair_weight[...], high.astype(bf16), preferred_element_type=f32)
        lower = jnp.dot(pair_weight[:80], low.astype(bf16), preferred_element_type=f32)
        total = upper[:ROWS] + upper[ROWS:] + lower[:ROWS]
        return jnp.concatenate([total[:, :LANES], total[:, LANES:]], 0)

    packed = []
    for half in range(2):
        whole = jnp.concatenate([section(4 * half + g) for g in range(4)], 1)
        packed.append(columns(whole, col_high, col_low))
    quads = [packed[half][f * ROWS : (f + 1) * ROWS] for f in range(2) for half in range(2)]
    main = [q[:, :LANES] for q in quads]
    extra = quads[0][:, LANES:]
    for j in range(1, 4):
        extra = extra + pltpu.roll(quads[j][:, LANES:], j, 1)
    for k in range(4):
        tail = None
        for p, plane in enumerate((2 * k, 2 * k + 1, NODES)):
            rows = slice(plane * 8, plane * 8 + 8)
            for j in range(4):
                start = plane_row(j, p)
                blocks[k, start : start + 8] = main[j][rows]
            piece = extra[rows]
            piece = piece if p == 0 else pltpu.roll(piece, 4 * p, 1)
            tail = piece if tail is None else tail + piece
        blocks[k, 64:72] = tail


def route_kernel(blocks, incoming, *outs):
    gz = lax.axis_index("gz")
    top = lax.broadcasted_iota(jnp.int32, (8, LANES), 0) == 0
    top = jnp.logical_and(top, lax.axis_index("gx") > 0)
    for k in range(4):
        which = lax.rem(gz + k, 4)
        out = outs[k]
        tail = None
        for p in range(3):
            for j in range(4):
                start = plane_row(j, p)
                if p < 2:
                    row = incoming[pl.ds(j * 8 + 2 * which + p, 1), :]
                else:
                    row = incoming[32 + j : 33 + j, :]
                if start < out.shape[0]:
                    own = blocks[which, start : start + 8]
                    out[start : start + 8] = own + jnp.where(top, row, 0.0)
            if p < 2:
                row = incoming[pl.ds(40 + 2 * which + p, 1), :]
            else:
                row = incoming[36:37, :]
            row = jnp.where(top, row, 0.0)
            row = row if p == 0 else pltpu.roll(row, 4 * p, 1)
            tail = row if tail is None else tail + row
        out[64:72] = blocks[which, 64:72] + tail


def combine_kernel(own, one, two, three, *rest):
    outs, slabs = rest[:4], rest[4]
    gy, gz = lax.axis_index("gy"), lax.axis_index("gz")
    for k, message in enumerate((own, one, two, three)):
        slabs[lax.rem(gz + 4 - k, 4), : message.shape[0]] = message[...]
    lane = lane_ids(8)
    for k in range(4):
        slab = lax.rem(gy + k, 4)
        before = lax.rem(slab + 3, 4)
        joins = jnp.logical_and(gz == 0, slab > 0)
        out = outs[k]
        for j in range(4):
            start = plane_row(j, 0)
            plane = slabs[before, plane_row(j, 2) : plane_row(j, 2) + 8]
            own = slabs[slab, start : start + 8]
            out[start : start + 8] = own + jnp.where(joins, plane, 0.0)
            start = plane_row(j, 1)
            out[start : start + 8] = slabs[slab, start : start + 8]
        tail = pltpu.roll(slabs[before, 64:72], LANES - 8, 1)
        tail = jnp.where(jnp.logical_and(joins, lane % COLS < 4), tail, 0.0)
        out[64:72] = slabs[slab, 64:72] + tail


def tension_kernel(
    own, one, two, three, troponin, tension, unbind, relax, bound_out, active_out, chunks
):
    gy = lax.axis_index("gy")
    for k, message in enumerate((own, one, two, three)):
        chunks[lax.rem(gy + 4 - k, 4)] = message[...]
    lane = lane_ids(8)
    quarter = lane // COLS
    odd = quarter % 2 == 1
    upper = quarter >= 2

    def turn(value, shift):
        shift = shift % LANES
        return value if shift == 0 else pltpu.roll(value, shift, 1)

    def spread(start):
        v = [chunks[c, start : start + 8] for c in range(4)]
        low = [jnp.where(upper, turn(v[c + 2], 64), v[c]) for c in range(2)]
        high = [jnp.where(upper, v[c + 2], turn(v[c], 64)) for c in range(2)]
        out = []
        for one, two in (low, high):
            out.append(jnp.where(odd, turn(two, COLS), one))
            out.append(jnp.where(odd, two, turn(one, -COLS)))
        return out

    def ends(group):
        total = None
        for c in range(3):
            part = turn(chunks[c, 64:72], COLS * (c + 1 - group))
            part = jnp.where(quarter == c + 1, part, 0.0)
            total = part if total is None else total + part
        return total

    starts = lane % COLS == 0
    last_columns = [ends(group) for group in range(4)]
    drives = {}
    for plane in range(2):
        for j in range(4):
            for group, value in enumerate(spread(j * 16 + plane * 8)):
                extra = turn(last_columns[group], -(4 * plane + j))
                value = value + jnp.where(starts, extra, 0.0)
                drives[j // 2, 4 * (j % 2) + group, plane] = value

    def drive(f, substep, plane):
        return drives[f, substep, plane]

    for plane in range(2):
        bound = troponin[:, plane, :]
        active = tension[:, plane, :]
        unbinding = unbind[:, plane, :]
        relaxing = step_size * relax[:, plane, :]
        for substep in range(SUBS):
            calcium_now = drive(0, substep, plane)
            squared = calcium_now * calcium_now
            binding = squared / (squared + half_square)
            bound = bound + step_size * (
                bind_rate * binding * (1.0 - bound) - unbinding * bound
            )
            active = active + relaxing * (
                peak_tension * drive(1, substep, plane) * bound - active
            )
        bound_out[:, plane, :] = bound
        active_out[:, plane, :] = active


def exchange(messages, axis):
    received = [messages[0]] + [None] * 3
    for k in range(1, 4):
        pairs = [(i, (i + k) % 4) for i in range(4)]
        received[k] = lax.ppermute(messages[k], axis, pairs)
    return received


def per_device(
    calcium,
    activation,
    element_first,
    offset_first,
    element_second,
    offset_second,
    element_third,
    offset_third,
    troponin,
    tension,
    unbind_rate,
    relax_rate,
):
    line = lambda n, kind: pltpu.VMEM((n,), kind)
    vectors = (
        element_first,
        offset_first,
        element_second,
        offset_second,
        element_third,
        offset_third,
    )
    far = [
        pltpu.with_memory_space_constraint(x, pltpu.HBM)
        for x in (calcium, activation) + vectors
    ]
    edge, *weights = pl.pallas_call(
        edge_kernel,
        in_specs=[pl.BlockSpec(memory_space=pltpu.HBM)] * 8,
        out_shape=[
            jax.ShapeDtypeStruct((48, LANES), f32),
            jax.ShapeDtypeStruct((16, LANES), f32),
            jax.ShapeDtypeStruct((16, LANES), f32),
            jax.ShapeDtypeStruct((512, 256), bf16),
            jax.ShapeDtypeStruct((512, 256), bf16),
        ],
        scratch_shapes=[line(x.shape[0], x.dtype) for x in vectors]
        + [
            pltpu.VMEM((2, SUBS, 32 - SURE, 32, LANES), f32),
            pltpu.VMEM((SURE // 2, 2, SUBS, 2, 32, LANES), f32),
            pltpu.VMEM((32, 2048), f32),
            pltpu.SemaphoreType.DMA((6,)),
            pltpu.SemaphoreType.DMA,
            pltpu.SemaphoreType.DMA((SURE // 2,)),
        ],
        compiler_params=pltpu.CompilerParams(vmem_limit_bytes=16 << 20),
        name="edge",
    )(*far)
    incoming = lax.ppermute(edge, "gx", [(i, (i + 1) % 8) for i in range(8)])
    blocks = pl.pallas_call(
        restrict_kernel,
        out_shape=jax.ShapeDtypeStruct((4, BLOCK, LANES), f32),
        scratch_shapes=[pltpu.VMEM((2 * ROWS, 1024), bf16)],
        compiler_params=pltpu.CompilerParams(vmem_limit_bytes=16 << 20),
        name="restrict",
    )(calcium, activation, *weights)
    small = pltpu.CompilerParams(vmem_limit_bytes=4 << 20)
    sizes = [PIECE if k == 1 else BLOCK for k in range(4)]
    message = [jax.ShapeDtypeStruct((n, LANES), f32) for n in sizes]
    messages = pl.pallas_call(route_kernel, out_shape=message, compiler_params=small, name="route")(
        blocks, incoming
    )
    messages = exchange(messages, "gz")
    piece = jax.ShapeDtypeStruct((PIECE, LANES), f32)
    pieces = pl.pallas_call(
        combine_kernel,
        out_shape=[piece] * 4,
        scratch_shapes=[pltpu.VMEM((4, BLOCK, LANES), f32)],
        compiler_params=small,
        name="combine",
    )(*messages)
    pieces = exchange(pieces, "gy")
    result = jax.ShapeDtypeStruct(troponin.shape, f32)
    return pl.pallas_call(
        tension_kernel,
        out_shape=[result, result],
        scratch_shapes=[pltpu.VMEM((4, PIECE, LANES), f32)],
        compiler_params=small,
        name="tension",
    )(*pieces, troponin, tension, unbind_rate, relax_rate)


def solution(mesh):
    node_spec = P("gx", ("gy", "gz"), None)
    return jax.shard_map(
        per_device,
        mesh=mesh,
        in_specs=(P(None, "gx", "gz", "gy"),) * 2 + (P(),) * 6 + (node_spec,) * 4,
        out_specs=(node_spec, node_spec),
        check_vma=False,
    )
```

```python
import jax
import jax.numpy as jnp
from jax import lax
from jax.experimental import pallas as pl
from jax.experimental.pallas import tpu as pltpu
from jax.sharding import PartitionSpec as P


step_size = 0.2
bind_rate = 2.0
peak_tension = 2.0
half_square = 0.25

f32 = jnp.float32
bf16 = jnp.bfloat16
LANES = 128
SUBS = 8
NODES = 8
COLS = 32
ROWS = 72
BLOCK = 104
SURE = 26
PIECE = 72


def hat(element, offset, first_node, rows):
    cells = element.shape[0]
    element = element.reshape(1, cells)
    offset = offset.reshape(1, cells)
    node = first_node + lax.broadcasted_iota(jnp.int32, (rows, cells), 0)
    raw = jnp.where(element == node, 1.0 - offset, 0.0) + jnp.where(
        element + 1 == node, offset, 0.0
    )
    return raw / jnp.sum(raw, axis=1, keepdims=True)


def halves(value):
    high = value.astype(bf16).astype(f32)
    return high, value - high


def plane_row(j, p):
    return j * 16 + p * 8 if p < 2 else PIECE + j * 8


def lane_ids(rows):
    return lax.broadcasted_iota(jnp.int32, (rows, LANES), 1)


def pick_lanes(values, index):
    return jnp.take_along_axis(values, index, axis=1, mode="promise_in_bounds")


def edge_kernel(
    calcium,
    activation,
    element_first,
    offset_first,
    element_second,
    offset_second,
    element_third,
    offset_third,
    edge,
    first_weight,
    depth_weight,
    col_high,
    col_low,
    elements_1,
    offsets_1,
    elements_2,
    offsets_2,
    elements_3,
    offsets_3,
    sure_cells,
    cells,
    sums,
    small_sems,
    sure_sem,
    cell_sems,
):
    gx, gy, gz = lax.axis_index("gx"), lax.axis_index("gy"), lax.axis_index("gz")
    small = [
        (element_first, elements_1),
        (offset_first, offsets_1),
        (element_third, elements_3),
        (offset_third, offsets_3),
        (element_second, elements_2),
        (offset_second, offsets_2),
    ]
    loads = [
        pltpu.make_async_copy(source, target, small_sems.at[n])
        for n, (source, target) in enumerate(small)
    ]
    fields = (calcium, activation)
    sure_copies = [
        pltpu.make_async_copy(field.at[:, SURE:], sure_cells.at[f], sure_sem)
        for f, field in enumerate(fields)
    ]
    for load in loads:
        load.start()
    passes_on = gx < 7

    @pl.when(passes_on)
    def _():
        for copy in sure_copies:
            copy.start()

    for load in loads[:4]:
        load.wait()

    first = hat(elements_1[...], offsets_1[...], gx * NODES, 16)
    own = jnp.where(gx >= 4, first[:, LANES:], first[:, :LANES])
    third = hat(elements_3[...], offsets_3[...], gz * NODES, 16)
    depth = pick_lanes(third, gz * 32 + lane_ids(16) % 32)
    first_weight[...] = own
    depth_weight[...] = depth

    place = lax.broadcasted_iota(jnp.int32, (1, 256), 1)
    earlier = jnp.logical_and(
        place // 32 == gx, elements_1[...].reshape(1, 256) < gx * NODES + NODES - 1
    )
    begin = jnp.sum(jnp.where(earlier, 1.0, 0.0)).astype(jnp.int32)

    count = jnp.where(passes_on, (SURE + 1 - begin) // 2, 0)

    def start(n, carry):
        for f, field in enumerate(fields):
            layers = pl.ds(SURE - 2 - 2 * n, 2)
            pltpu.make_async_copy(
                field.at[:, layers], cells.at[n, f], cell_sems.at[n]
            ).start()
        return carry

    lax.fori_loop(0, count, start, 0)
    loads[4].wait()
    loads[5].wait()
    second = hat(elements_2[...], offsets_2[...], gy * COLS, 40)
    chunk = second[:, :LANES]
    for c in range(1, 4):
        chunk = jnp.where(gy == c, second[:, c * LANES : (c + 1) * LANES], chunk)
    full = jnp.concatenate([chunk, jnp.zeros((LANES - 40, LANES), f32)], 0)
    turned = full.T
    lane = lane_ids(LANES)
    for group in range(4):
        first_lane = group * COLS
        main = turned if group == 0 else pltpu.roll(turned, first_lane, 1)
        main = jnp.where(lane // COLS == group, main, 0.0)
        shift = (first_lane - COLS) % LANES
        extra = turned if shift == 0 else pltpu.roll(turned, shift, 1)
        extra = jnp.where(lane == first_lane, extra, 0.0)
        high, low = halves(jnp.concatenate([main, extra], 1))
        rows = slice(group * LANES, (group + 1) * LANES)
        col_high[rows] = high.astype(bf16)
        col_low[rows] = low.astype(bf16)

    @pl.when(passes_on)
    def _():
        layer = jnp.broadcast_to(own[NODES : NODES + 1], (8, LANES))

        def cell_weight(x):
            index = jnp.full((8, LANES), lax.rem(gx, 4) * 32 + x, jnp.int32)
            return jnp.concatenate([pick_lanes(layer, index)] * 4, 0)

        slots = [(f, t, (f * SUBS + t) * LANES) for f in range(2) for t in range(SUBS)]
        pltpu.make_async_copy(sure_cells, sure_cells, sure_sem).wait()
        sure_weights = [cell_weight(x) for x in range(SURE, 32)]
        for f, t, column in slots:
            total = None
            for n, weight in enumerate(sure_weights):
                part = weight * sure_cells[f, t, n]
                total = part if total is None else total + part
            sums[:, column : column + LANES] = total

        def add(n, carry):
            pltpu.make_async_copy(cells.at[n], cells.at[n], cell_sems.at[n]).wait()
            pair = [cell_weight(SURE - 2 - 2 * n + i) for i in range(2)]
            for f, t, column in slots:
                part = pair[0] * cells[n, f, t, 0] + pair[1] * cells[n, f, t, 1]
                sums[:, column : column + LANES] += part
            return carry

        lax.fori_loop(0, count, add, 0)

        depth_high, depth_low = halves(depth[:, :32])
        weights = jnp.concatenate([depth_high, depth_low], 0).astype(bf16)
        high, low = halves(sums[...])
        upper = jnp.dot(weights, high.astype(bf16), preferred_element_type=f32)
        lower = jnp.dot(weights[:16], low.astype(bf16), preferred_element_type=f32)
        planes = upper[:16] + upper[16:] + lower
        whole = jnp.concatenate([planes[:, j * 512 : (j + 1) * 512] for j in range(4)], 0)
        result = columns(whole, col_high, col_low)
        quads = [result[j * 16 : j * 16 + 16] for j in range(4)]
        extra = quads[0][:, LANES:]
        for j in range(1, 4):
            extra = extra + pltpu.roll(quads[j][:, LANES:], j, 1)
        for j in range(4):
            edge[j * 8 : j * 8 + 8] = quads[j][:8, :LANES]
        corners = [q[8:9, :LANES] for q in quads] + [extra[8:9]]
        edge[32:40] = jnp.concatenate(corners + [jnp.zeros((3, LANES), f32)], 0)
        edge[40:48] = extra[:8]


def columns(whole, col_high, col_low):
    high, low = halves(whole)
    high, low = high.astype(bf16), low.astype(bf16)
    return (
        jnp.dot(high, col_high[...], preferred_element_type=f32)
        + jnp.dot(low, col_high[...], preferred_element_type=f32)
        + jnp.dot(high, col_low[...], preferred_element_type=f32)
    )


def restrict_kernel(
    calcium, activation, first_weight, depth_weight, col_high, col_low, blocks, pair_weight
):
    gx = lax.axis_index("gx")
    lane = lane_ids(16)
    own, depth = first_weight[...], depth_weight[...]
    for tile in range(8):
        row = pick_lanes(own, lax.rem(gx, 4) * 32 + 4 * tile + lane // 32)
        parts = [depth[b : b + 1] * row[:NODES] for b in range(NODES + 1)]
        both = jnp.concatenate(halves(jnp.concatenate(parts, 0)), 0)
        pair_weight[:, tile * LANES : (tile + 1) * LANES] = both.astype(bf16)

    cells = 32 * 32

    def section(t):
        field = jnp.concatenate(
            [calcium[t].reshape(cells, LANES), activation[t].reshape(cells, LANES)], 1
        )
        high, low = halves(field)
        upper = jnp.dot(pair_weight[...], high.astype(bf16), preferred_element_type=f32)
        lower = jnp.dot(pair_weight[:80], low.astype(bf16), preferred_element_type=f32)
        total = upper[:ROWS] + upper[ROWS:] + lower[:ROWS]
        return jnp.concatenate([total[:, :LANES], total[:, LANES:]], 0)

    packed = []
    for half in range(2):
        whole = jnp.concatenate([section(4 * half + g) for g in range(4)], 1)
        packed.append(columns(whole, col_high, col_low))
    quads = [packed[half][f * ROWS : (f + 1) * ROWS] for f in range(2) for half in range(2)]
    main = [q[:, :LANES] for q in quads]
    extra = quads[0][:, LANES:]
    for j in range(1, 4):
        extra = extra + pltpu.roll(quads[j][:, LANES:], j, 1)
    for k in range(4):
        tail = None
        for p, plane in enumerate((2 * k, 2 * k + 1, NODES)):
            rows = slice(plane * 8, plane * 8 + 8)
            for j in range(4):
                start = plane_row(j, p)
                blocks[k, start : start + 8] = main[j][rows]
            piece = extra[rows]
            piece = piece if p == 0 else pltpu.roll(piece, 4 * p, 1)
            tail = piece if tail is None else tail + piece
        blocks[k, 64:72] = tail


def route_kernel(blocks, incoming, *outs):
    gz = lax.axis_index("gz")
    top = lax.broadcasted_iota(jnp.int32, (8, LANES), 0) == 0
    top = jnp.logical_and(top, lax.axis_index("gx") > 0)
    for k in range(4):
        which = lax.rem(gz + k, 4)
        out = outs[k]
        tail = None
        for p in range(3):
            for j in range(4):
                start = plane_row(j, p)
                if p < 2:
                    row = incoming[pl.ds(j * 8 + 2 * which + p, 1), :]
                else:
                    row = incoming[32 + j : 33 + j, :]
                if start < out.shape[0]:
                    own = blocks[which, start : start + 8]
                    out[start : start + 8] = own + jnp.where(top, row, 0.0)
            if p < 2:
                row = incoming[pl.ds(40 + 2 * which + p, 1), :]
            else:
                row = incoming[36:37, :]
            row = jnp.where(top, row, 0.0)
            row = row if p == 0 else pltpu.roll(row, 4 * p, 1)
            tail = row if tail is None else tail + row
        out[64:72] = blocks[which, 64:72] + tail


def combine_kernel(own, one, two, three, *rest):
    outs, slabs = rest[:4], rest[4]
    gy, gz = lax.axis_index("gy"), lax.axis_index("gz")
    for k, message in enumerate((own, one, two, three)):
        slabs[lax.rem(gz + 4 - k, 4), : message.shape[0]] = message[...]
    lane = lane_ids(8)
    for k in range(4):
        slab = lax.rem(gy + k, 4)
        before = lax.rem(slab + 3, 4)
        joins = jnp.logical_and(gz == 0, slab > 0)
        out = outs[k]
        for j in range(4):
            start = plane_row(j, 0)
            plane = slabs[before, plane_row(j, 2) : plane_row(j, 2) + 8]
            own = slabs[slab, start : start + 8]
            out[start : start + 8] = own + jnp.where(joins, plane, 0.0)
            start = plane_row(j, 1)
            out[start : start + 8] = slabs[slab, start : start + 8]
        tail = pltpu.roll(slabs[before, 64:72], LANES - 8, 1)
        tail = jnp.where(jnp.logical_and(joins, lane % COLS < 4), tail, 0.0)
        out[64:72] = slabs[slab, 64:72] + tail


def tension_kernel(
    own, one, two, three, troponin, tension, unbind, relax, bound_out, active_out, chunks
):
    gy = lax.axis_index("gy")
    for k, message in enumerate((own, one, two, three)):
        chunks[lax.rem(gy + 4 - k, 4)] = message[...]
    lane = lane_ids(8)
    quarter = lane // COLS
    odd = quarter % 2 == 1
    upper = quarter >= 2

    def turn(value, shift):
        shift = shift % LANES
        return value if shift == 0 else pltpu.roll(value, shift, 1)

    def spread(start):
        v = [chunks[c, start : start + 8] for c in range(4)]
        low = [jnp.where(upper, turn(v[c + 2], 64), v[c]) for c in range(2)]
        high = [jnp.where(upper, v[c + 2], turn(v[c], 64)) for c in range(2)]
        out = []
        for one, two in (low, high):
            out.append(jnp.where(odd, turn(two, COLS), one))
            out.append(jnp.where(odd, two, turn(one, -COLS)))
        return out

    def ends(group):
        total = None
        for c in range(3):
            part = turn(chunks[c, 64:72], COLS * (c + 1 - group))
            part = jnp.where(quarter == c + 1, part, 0.0)
            total = part if total is None else total + part
        return total

    starts = lane % COLS == 0
    last_columns = [ends(group) for group in range(4)]
    drives = {}
    for plane in range(2):
        for j in range(4):
            for group, value in enumerate(spread(j * 16 + plane * 8)):
                extra = turn(last_columns[group], -(4 * plane + j))
                value = value + jnp.where(starts, extra, 0.0)
                drives[j // 2, 4 * (j % 2) + group, plane] = value

    def drive(f, substep, plane):
        return drives[f, substep, plane]

    for plane in range(2):
        bound = troponin[:, plane, :]
        active = tension[:, plane, :]
        unbinding = unbind[:, plane, :]
        relaxing = step_size * relax[:, plane, :]
        for substep in range(SUBS):
            calcium_now = drive(0, substep, plane)
            squared = calcium_now * calcium_now
            binding = squared / (squared + half_square)
            bound = bound + step_size * (
                bind_rate * binding * (1.0 - bound) - unbinding * bound
            )
            active = active + relaxing * (
                peak_tension * drive(1, substep, plane) * bound - active
            )
        bound_out[:, plane, :] = bound
        active_out[:, plane, :] = active


def exchange(messages, axis):
    received = [messages[0]] + [None] * 3
    for k in range(1, 4):
        pairs = [(i, (i + k) % 4) for i in range(4)]
        received[k] = lax.ppermute(messages[k], axis, pairs)
    return received


def per_device(
    calcium,
    activation,
    element_first,
    offset_first,
    element_second,
    offset_second,
    element_third,
    offset_third,
    troponin,
    tension,
    unbind_rate,
    relax_rate,
):
    line = lambda n, kind: pltpu.VMEM((n,), kind)
    vectors = (
        element_first,
        offset_first,
        element_second,
        offset_second,
        element_third,
        offset_third,
    )
    far = [
        pltpu.with_memory_space_constraint(x, pltpu.HBM)
        for x in (calcium, activation) + vectors
    ]
    edge, *weights = pl.pallas_call(
        edge_kernel,
        in_specs=[pl.BlockSpec(memory_space=pltpu.HBM)] * 8,
        out_shape=[
            jax.ShapeDtypeStruct((48, LANES), f32),
            jax.ShapeDtypeStruct((16, LANES), f32),
            jax.ShapeDtypeStruct((16, LANES), f32),
            jax.ShapeDtypeStruct((512, 256), bf16),
            jax.ShapeDtypeStruct((512, 256), bf16),
        ],
        scratch_shapes=[line(x.shape[0], x.dtype) for x in vectors]
        + [
            pltpu.VMEM((2, SUBS, 32 - SURE, 32, LANES), f32),
            pltpu.VMEM((SURE // 2, 2, SUBS, 2, 32, LANES), f32),
            pltpu.VMEM((32, 2048), f32),
            pltpu.SemaphoreType.DMA((6,)),
            pltpu.SemaphoreType.DMA,
            pltpu.SemaphoreType.DMA((SURE // 2,)),
        ],
        compiler_params=pltpu.CompilerParams(vmem_limit_bytes=16 << 20),
        name="edge",
    )(*far)
    incoming = lax.ppermute(edge, "gx", [(i, (i + 1) % 8) for i in range(8)])
    blocks = pl.pallas_call(
        restrict_kernel,
        out_shape=jax.ShapeDtypeStruct((4, BLOCK, LANES), f32),
        scratch_shapes=[pltpu.VMEM((2 * ROWS, 1024), bf16)],
        compiler_params=pltpu.CompilerParams(vmem_limit_bytes=16 << 20),
        name="restrict",
    )(calcium, activation, *weights)
    small = pltpu.CompilerParams(vmem_limit_bytes=4 << 20)
    sizes = [PIECE if k == 1 else BLOCK for k in range(4)]
    message = [jax.ShapeDtypeStruct((n, LANES), f32) for n in sizes]
    messages = pl.pallas_call(route_kernel, out_shape=message, compiler_params=small, name="route")(
        blocks, incoming
    )
    messages = exchange(messages, "gz")
    piece = jax.ShapeDtypeStruct((PIECE, LANES), f32)
    pieces = pl.pallas_call(
        combine_kernel,
        out_shape=[piece] * 4,
        scratch_shapes=[pltpu.VMEM((4, BLOCK, LANES), f32)],
        compiler_params=small,
        name="combine",
    )(*messages)
    pieces = exchange(pieces, "gy")
    result = jax.ShapeDtypeStruct(troponin.shape, f32)
    return pl.pallas_call(
        tension_kernel,
        out_shape=[result, result],
        scratch_shapes=[pltpu.VMEM((4, PIECE, LANES), f32)],
        compiler_params=small,
        name="tension",
    )(*pieces, troponin, tension, unbind_rate, relax_rate)


def solution(mesh):
    node_spec = P("gx", ("gy", "gz"), None)
    return jax.shard_map(
        per_device,
        mesh=mesh,
        in_specs=(P(None, "gx", "gz", "gy"),) * 2 + (P(),) * 6 + (node_spec,) * 4,
        out_specs=(node_spec, node_spec),
        check_vma=False,
    )
```

```python
import jax
import jax.numpy as jnp
from jax import lax
from jax.experimental import pallas as pl
from jax.experimental.pallas import tpu as pltpu
from jax.sharding import PartitionSpec as P


step_size = 0.2
bind_rate = 2.0
peak_tension = 2.0
half_square = 0.25

f32 = jnp.float32
bf16 = jnp.bfloat16
LANES = 128
SUBS = 8
NODES = 8
COLS = 32
ROWS = 72
BLOCK = 104
SURE = 26
PAIRS = (SURE + 1 - (NODES - 1)) // 2
PIECE = 72


def hat(element, offset, first_node, rows):
    cells = element.shape[0]
    element = element.reshape(1, cells)
    offset = offset.reshape(1, cells)
    node = first_node + lax.broadcasted_iota(jnp.int32, (rows, cells), 0)
    raw = jnp.where(element == node, 1.0 - offset, 0.0) + jnp.where(
        element + 1 == node, offset, 0.0
    )
    return raw / jnp.sum(raw, axis=1, keepdims=True)


def halves(value):
    high = value.astype(bf16).astype(f32)
    return high, value - high


def plane_row(j, p):
    return j * 16 + p * 8 if p < 2 else PIECE + j * 8


def lane_ids(rows):
    return lax.broadcasted_iota(jnp.int32, (rows, LANES), 1)


def pick_lanes(values, index):
    return jnp.take_along_axis(values, index, axis=1, mode="promise_in_bounds")


def edge_kernel(
    calcium,
    activation,
    element_first,
    offset_first,
    element_second,
    offset_second,
    element_third,
    offset_third,
    edge,
    first_weight,
    depth_weight,
    col_high,
    col_low,
    elements_1,
    offsets_1,
    elements_2,
    offsets_2,
    elements_3,
    offsets_3,
    sure_cells,
    cells,
    sums,
    small_sems,
    sure_sem,
    cell_sems,
):
    gx, gy, gz = lax.axis_index("gx"), lax.axis_index("gy"), lax.axis_index("gz")
    small = [
        (element_first, elements_1),
        (offset_first, offsets_1),
        (element_third, elements_3),
        (offset_third, offsets_3),
        (element_second, elements_2),
        (offset_second, offsets_2),
    ]
    loads = [
        pltpu.make_async_copy(source, target, small_sems.at[n])
        for n, (source, target) in enumerate(small)
    ]
    fields = (calcium, activation)
    sure_copies = [
        pltpu.make_async_copy(field.at[:, SURE:], sure_cells.at[f], sure_sem)
        for f, field in enumerate(fields)
    ]
    for load in loads:
        load.start()
    passes_on = gx < 7

    @pl.when(passes_on)
    def _():
        for copy in sure_copies:
            copy.start()

    for load in loads[:4]:
        load.wait()

    first = hat(elements_1[...], offsets_1[...], gx * NODES, 16)
    own = jnp.where(gx >= 4, first[:, LANES:], first[:, :LANES])
    third = hat(elements_3[...], offsets_3[...], gz * NODES, 16)
    depth = pick_lanes(third, gz * 32 + lane_ids(16) % 32)
    first_weight[...] = own
    depth_weight[...] = depth

    place = lax.broadcasted_iota(jnp.int32, (1, 256), 1)
    earlier = jnp.logical_and(
        place // 32 == gx, elements_1[...].reshape(1, 256) < gx * NODES + NODES - 1
    )
    begin = jnp.sum(jnp.where(earlier, 1.0, 0.0)).astype(jnp.int32)

    count = jnp.where(passes_on, (SURE + 1 - begin) // 2, 0)

    def start(n, carry):
        for f, field in enumerate(fields):
            layers = pl.ds(SURE - 2 - 2 * n, 2)
            pltpu.make_async_copy(
                field.at[:, layers], cells.at[n, f], cell_sems.at[n]
            ).start()
        return carry

    lax.fori_loop(0, count, start, 0)
    loads[4].wait()
    loads[5].wait()
    second = hat(elements_2[...], offsets_2[...], gy * COLS, 40)
    chunk = second[:, :LANES]
    for c in range(1, 4):
        chunk = jnp.where(gy == c, second[:, c * LANES : (c + 1) * LANES], chunk)
    full = jnp.concatenate([chunk, jnp.zeros((LANES - 40, LANES), f32)], 0)
    turned = full.T
    lane = lane_ids(LANES)
    for group in range(4):
        first_lane = group * COLS
        main = turned if group == 0 else pltpu.roll(turned, first_lane, 1)
        main = jnp.where(lane // COLS == group, main, 0.0)
        shift = (first_lane - COLS) % LANES
        extra = turned if shift == 0 else pltpu.roll(turned, shift, 1)
        extra = jnp.where(lane == first_lane, extra, 0.0)
        high, low = halves(jnp.concatenate([main, extra], 1))
        rows = slice(group * LANES, (group + 1) * LANES)
        col_high[rows] = high.astype(bf16)
        col_low[rows] = low.astype(bf16)

    @pl.when(passes_on)
    def _():
        layer = jnp.broadcast_to(own[NODES : NODES + 1], (8, LANES))

        def cell_weight(x):
            index = jnp.full((8, LANES), lax.rem(gx, 4) * 32 + x, jnp.int32)
            return jnp.concatenate([pick_lanes(layer, index)] * 4, 0)

        slots = [(f, t, (f * SUBS + t) * LANES) for f in range(2) for t in range(SUBS)]
        pltpu.make_async_copy(sure_cells, sure_cells, sure_sem).wait()
        sure_weights = [cell_weight(x) for x in range(SURE, 32)]
        for f, t, column in slots:
            total = None
            for n, weight in enumerate(sure_weights):
                part = weight * sure_cells[f, t, n]
                total = part if total is None else total + part
            sums[:, column : column + LANES] = total

        def add(n, carry):
            pltpu.make_async_copy(cells.at[n], cells.at[n], cell_sems.at[n]).wait()
            pair = [cell_weight(SURE - 2 - 2 * n + i) for i in range(2)]
            for f, t, column in slots:
                part = pair[0] * cells[n, f, t, 0] + pair[1] * cells[n, f, t, 1]
                sums[:, column : column + LANES] += part
            return carry

        lax.fori_loop(0, count, add, 0)

        depth_high, depth_low = halves(depth[:, :32])
        weights = jnp.concatenate([depth_high, depth_low], 0).astype(bf16)
        high, low = halves(sums[...])
        upper = jnp.dot(weights, high.astype(bf16), preferred_element_type=f32)
        lower = jnp.dot(weights[:16], low.astype(bf16), preferred_element_type=f32)
        planes = upper[:16] + upper[16:] + lower
        whole = jnp.concatenate([planes[:, j * 512 : (j + 1) * 512] for j in range(4)], 0)
        result = columns(whole, col_high, col_low)
        quads = [result[j * 16 : j * 16 + 16] for j in range(4)]
        extra = quads[0][:, LANES:]
        for j in range(1, 4):
            extra = extra + pltpu.roll(quads[j][:, LANES:], j, 1)
        for j in range(4):
            edge[j * 8 : j * 8 + 8] = quads[j][:8, :LANES]
        corners = [q[8:9, :LANES] for q in quads] + [extra[8:9]]
        edge[32:40] = jnp.concatenate(corners + [jnp.zeros((3, LANES), f32)], 0)
        edge[40:48] = extra[:8]


def columns(whole, col_high, col_low):
    high, low = halves(whole)
    high, low = high.astype(bf16), low.astype(bf16)
    return (
        jnp.dot(high, col_high[...], preferred_element_type=f32)
        + jnp.dot(low, col_high[...], preferred_element_type=f32)
        + jnp.dot(high, col_low[...], preferred_element_type=f32)
    )


def restrict_kernel(
    calcium, activation, first_weight, depth_weight, col_high, col_low, blocks, pair_weight
):
    gx = lax.axis_index("gx")
    lane = lane_ids(16)
    own, depth = first_weight[...], depth_weight[...]
    for tile in range(8):
        row = pick_lanes(own, lax.rem(gx, 4) * 32 + 4 * tile + lane // 32)
        parts = [depth[b : b + 1] * row[:NODES] for b in range(NODES + 1)]
        both = jnp.concatenate(halves(jnp.concatenate(parts, 0)), 0)
        pair_weight[:, tile * LANES : (tile + 1) * LANES] = both.astype(bf16)

    cells = 32 * 32

    def section(t):
        field = jnp.concatenate(
            [calcium[t].reshape(cells, LANES), activation[t].reshape(cells, LANES)], 1
        )
        high, low = halves(field)
        upper = jnp.dot(pair_weight[...], high.astype(bf16), preferred_element_type=f32)
        lower = jnp.dot(pair_weight[:80], low.astype(bf16), preferred_element_type=f32)
        total = upper[:ROWS] + upper[ROWS:] + lower[:ROWS]
        return jnp.concatenate([total[:, :LANES], total[:, LANES:]], 0)

    packed = []
    for half in range(2):
        whole = jnp.concatenate([section(4 * half + g) for g in range(4)], 1)
        packed.append(columns(whole, col_high, col_low))
    quads = [packed[half][f * ROWS : (f + 1) * ROWS] for f in range(2) for half in range(2)]
    main = [q[:, :LANES] for q in quads]
    extra = quads[0][:, LANES:]
    for j in range(1, 4):
        extra = extra + pltpu.roll(quads[j][:, LANES:], j, 1)
    for k in range(4):
        tail = None
        for p, plane in enumerate((2 * k, 2 * k + 1, NODES)):
            rows = slice(plane * 8, plane * 8 + 8)
            for j in range(4):
                start = plane_row(j, p)
                blocks[k, start : start + 8] = main[j][rows]
            piece = extra[rows]
            piece = piece if p == 0 else pltpu.roll(piece, 4 * p, 1)
            tail = piece if tail is None else tail + piece
        blocks[k, 64:72] = tail


def route_kernel(blocks, incoming, *outs):
    gz = lax.axis_index("gz")
    top = lax.broadcasted_iota(jnp.int32, (8, LANES), 0) == 0
    top = jnp.logical_and(top, lax.axis_index("gx") > 0)
    for k in range(4):
        which = lax.rem(gz + k, 4)
        out = outs[k]
        tail = None
        for p in range(3):
            for j in range(4):
                start = plane_row(j, p)
                if p < 2:
                    row = incoming[pl.ds(j * 8 + 2 * which + p, 1), :]
                else:
                    row = incoming[32 + j : 33 + j, :]
                if start < out.shape[0]:
                    own = blocks[which, start : start + 8]
                    out[start : start + 8] = own + jnp.where(top, row, 0.0)
            if p < 2:
                row = incoming[pl.ds(40 + 2 * which + p, 1), :]
            else:
                row = incoming[36:37, :]
            row = jnp.where(top, row, 0.0)
            row = row if p == 0 else pltpu.roll(row, 4 * p, 1)
            tail = row if tail is None else tail + row
        out[64:72] = blocks[which, 64:72] + tail


def combine_kernel(own, one, two, three, *rest):
    outs, slabs = rest[:4], rest[4]
    gy, gz = lax.axis_index("gy"), lax.axis_index("gz")
    for k, message in enumerate((own, one, two, three)):
        slabs[lax.rem(gz + 4 - k, 4), : message.shape[0]] = message[...]
    lane = lane_ids(8)
    for k in range(4):
        slab = lax.rem(gy + k, 4)
        before = lax.rem(slab + 3, 4)
        joins = jnp.logical_and(gz == 0, slab > 0)
        out = outs[k]
        for j in range(4):
            start = plane_row(j, 0)
            plane = slabs[before, plane_row(j, 2) : plane_row(j, 2) + 8]
            own = slabs[slab, start : start + 8]
            out[start : start + 8] = own + jnp.where(joins, plane, 0.0)
            start = plane_row(j, 1)
            out[start : start + 8] = slabs[slab, start : start + 8]
        tail = pltpu.roll(slabs[before, 64:72], LANES - 8, 1)
        tail = jnp.where(jnp.logical_and(joins, lane % COLS < 4), tail, 0.0)
        out[64:72] = slabs[slab, 64:72] + tail


def tension_kernel(
    own, one, two, three, troponin, tension, unbind, relax, bound_out, active_out, chunks
):
    gy = lax.axis_index("gy")
    for k, message in enumerate((own, one, two, three)):
        chunks[lax.rem(gy + 4 - k, 4)] = message[...]
    lane = lane_ids(8)
    quarter = lane // COLS
    odd = quarter % 2 == 1
    upper = quarter >= 2

    def turn(value, shift):
        shift = shift % LANES
        return value if shift == 0 else pltpu.roll(value, shift, 1)

    def spread(start):
        v = [chunks[c, start : start + 8] for c in range(4)]
        low = [jnp.where(upper, turn(v[c + 2], 64), v[c]) for c in range(2)]
        high = [jnp.where(upper, v[c + 2], turn(v[c], 64)) for c in range(2)]
        out = []
        for one, two in (low, high):
            out.append(jnp.where(odd, turn(two, COLS), one))
            out.append(jnp.where(odd, two, turn(one, -COLS)))
        return out

    def ends(group):
        total = None
        for c in range(3):
            part = turn(chunks[c, 64:72], COLS * (c + 1 - group))
            part = jnp.where(quarter == c + 1, part, 0.0)
            total = part if total is None else total + part
        return total

    starts = lane % COLS == 0
    last_columns = [ends(group) for group in range(4)]
    drives = {}
    for plane in range(2):
        for j in range(4):
            for group, value in enumerate(spread(j * 16 + plane * 8)):
                extra = turn(last_columns[group], -(4 * plane + j))
                value = value + jnp.where(starts, extra, 0.0)
                drives[j // 2, 4 * (j % 2) + group, plane] = value

    def drive(f, substep, plane):
        return drives[f, substep, plane]

    for plane in range(2):
        bound = troponin[:, plane, :]
        active = tension[:, plane, :]
        unbinding = unbind[:, plane, :]
        relaxing = step_size * relax[:, plane, :]
        for substep in range(SUBS):
            calcium_now = drive(0, substep, plane)
            squared = calcium_now * calcium_now
            binding = squared / (squared + half_square)
            bound = bound + step_size * (
                bind_rate * binding * (1.0 - bound) - unbinding * bound
            )
            active = active + relaxing * (
                peak_tension * drive(1, substep, plane) * bound - active
            )
        bound_out[:, plane, :] = bound
        active_out[:, plane, :] = active


def exchange(messages, axis):
    received = [messages[0]] + [None] * 3
    for k in range(1, 4):
        pairs = [(i, (i + k) % 4) for i in range(4)]
        received[k] = lax.ppermute(messages[k], axis, pairs)
    return received


def per_device(
    calcium,
    activation,
    element_first,
    offset_first,
    element_second,
    offset_second,
    element_third,
    offset_third,
    troponin,
    tension,
    unbind_rate,
    relax_rate,
):
    line = lambda n, kind: pltpu.VMEM((n,), kind)
    vectors = (
        element_first,
        offset_first,
        element_second,
        offset_second,
        element_third,
        offset_third,
    )
    far = [
        pltpu.with_memory_space_constraint(x, pltpu.HBM)
        for x in (calcium, activation) + vectors
    ]
    edge, *weights = pl.pallas_call(
        edge_kernel,
        in_specs=[pl.BlockSpec(memory_space=pltpu.HBM)] * 8,
        out_shape=[
            jax.ShapeDtypeStruct((48, LANES), f32),
            jax.ShapeDtypeStruct((16, LANES), f32),
            jax.ShapeDtypeStruct((16, LANES), f32),
            jax.ShapeDtypeStruct((512, 256), bf16),
            jax.ShapeDtypeStruct((512, 256), bf16),
        ],
        scratch_shapes=[line(x.shape[0], x.dtype) for x in vectors]
        + [
            pltpu.VMEM((2, SUBS, 32 - SURE, 32, LANES), f32),
            pltpu.VMEM((PAIRS, 2, SUBS, 2, 32, LANES), f32),
            pltpu.VMEM((32, 2048), f32),
            pltpu.SemaphoreType.DMA((6,)),
            pltpu.SemaphoreType.DMA,
            pltpu.SemaphoreType.DMA((PAIRS,)),
        ],
        compiler_params=pltpu.CompilerParams(vmem_limit_bytes=16 << 20),
        name="edge",
    )(*far)
    incoming = lax.ppermute(edge, "gx", [(i, (i + 1) % 8) for i in range(8)])
    blocks = pl.pallas_call(
        restrict_kernel,
        out_shape=jax.ShapeDtypeStruct((4, BLOCK, LANES), f32),
        scratch_shapes=[pltpu.VMEM((2 * ROWS, 1024), bf16)],
        compiler_params=pltpu.CompilerParams(vmem_limit_bytes=16 << 20),
        name="restrict",
    )(calcium, activation, *weights)
    small = pltpu.CompilerParams(vmem_limit_bytes=4 << 20)
    sizes = [PIECE if k == 1 else BLOCK for k in range(4)]
    message = [jax.ShapeDtypeStruct((n, LANES), f32) for n in sizes]
    messages = pl.pallas_call(route_kernel, out_shape=message, compiler_params=small, name="route")(
        blocks, incoming
    )
    messages = exchange(messages, "gz")
    piece = jax.ShapeDtypeStruct((PIECE, LANES), f32)
    pieces = pl.pallas_call(
        combine_kernel,
        out_shape=[piece] * 4,
        scratch_shapes=[pltpu.VMEM((4, BLOCK, LANES), f32)],
        compiler_params=small,
        name="combine",
    )(*messages)
    pieces = exchange(pieces, "gy")
    result = jax.ShapeDtypeStruct(troponin.shape, f32)
    return pl.pallas_call(
        tension_kernel,
        out_shape=[result, result],
        scratch_shapes=[pltpu.VMEM((4, PIECE, LANES), f32)],
        compiler_params=small,
        name="tension",
    )(*pieces, troponin, tension, unbind_rate, relax_rate)


def solution(mesh):
    node_spec = P("gx", ("gy", "gz"), None)
    return jax.shard_map(
        per_device,
        mesh=mesh,
        in_specs=(P(None, "gx", "gz", "gy"),) * 2 + (P(),) * 6 + (node_spec,) * 4,
        out_specs=(node_spec, node_spec),
        check_vma=False,
    )
```
